256 devices in a mesh: path: 64 (over z, y, core), dim: 4 (over x).
Axes of the slice: x: 4, y: 4, z: 8, core: 2. Of those that a mesh axis runs over, the one named last changes fastest.
Arguments:
- inner_noise: bfloat16 [512, 1000, 512], P('path', 'dim'), may hold values from -6 to 6
- outer_noise: bfloat16 [1000, 512], P('dim'), may hold values from -6 to 6
- start: float32 [1000], P('dim'), may hold values from 0.8 to 1.25
- vol: float32 [1000], P('dim'), may hold values from 0.1 to 0.4
- times: float32 [512], replicated, may hold values from 0.1 to 0.9
Outputs:
- root_value: float32 [1], replicated
- root_grad: float32 [1000], P('dim')
- point_value: float32 [512], P('path')
- point_grad: float32 [1000, 512], P('dim', 'path')
The draws below stay inside these ranges and needn't reach their ends.
All inputs are finite; a program needn't handle non-finite values.
Results may differ from the reference program's by a relative error of at most 0.0003.
Values sent between devices are 32-bit elements; how exact they have to be, the bound alone decides.
A program may use at most 64 MiB of HBM per device.

```python
import math
import jax
import jax.numpy as jnp
from jax import lax

D = 1000
M = 512
K = 512


def shard_levels(rng, shape, split, low, high):
    gain = 1.0
    for dim, blocks in split:
        steps = jax.random.uniform(jax.random.fold_in(jax.random.fold_in(rng, 6), dim), (blocks,), jnp.float32, low / len(split), high / len(split))
        gain = gain * jnp.repeat(jnp.exp(steps), shape[dim] // blocks).reshape((-1,) + (1,) * (len(shape) - 1 - dim))
    return gain


def centred(own_key, shape, width, most, pieces=(), held_as=jnp.bfloat16):
    factor_of = shard_levels(own_key, shape, pieces, -0.22, 0.18) if pieces else 1.0
    result = jax.random.normal(own_key, shape, jnp.float32) * width * factor_of
    return jnp.minimum(jnp.maximum(result, -most), most).astype(held_as)


def setup_inputs(seed: int = 0) -> dict:
    key_list = jax.random.split(jax.random.key(seed), 6)
    return {
        "inner_noise": centred(key_list[0], (K, D, M), 1.0, 6.0, ((0, 64), (1, 4))),
        "outer_noise": centred(key_list[1], (D, M), 1.0, 6.0, ((0, 4),)),
        "start": jnp.clip(jnp.exp(math.log(1.25) - 0.4462871 * jax.random.uniform(key_list[2], (D,), jnp.float32) ** shard_levels(key_list[2], (D,), ((0, 4),), -0.2, 0.2)), 0.8, 1.25),
        "vol": jnp.clip(jnp.exp(math.log(0.4) - 1.3862944 * jax.random.uniform(key_list[3], (D,), jnp.float32) ** shard_levels(key_list[3], (D,), ((0, 4),), -0.2, 0.2)), 0.1, 0.4),
        "times": jnp.clip(jax.random.uniform(key_list[4], (M,), jnp.float32, 0.1, 0.9), 0.1, 0.9),
    }


drift = 0.02
delta = 2.0 / 3.0
rate_free = 0.02
gamma_high = 0.2
gamma_low = 0.02
value_high = 0.4
value_low = 0.7

def driver_of(value):
    slope = jnp.clip((value - value_high) / (value_low - value_high), 0.0, 1.0)
    quota = gamma_high + (gamma_low - gamma_high) * slope
    return -(1.0 - delta) * quota * value - rate_free * value

def reference(inner_noise, outer_noise, start, vol, times):
    tau = 1.0 - times
    outer = outer_noise.astype(jnp.float32)
    mean_rate = (drift - 0.5 * vol * vol)[:, None]
    outer_state = start[:, None] * jnp.exp(mean_rate * times[None, :] + vol[:, None] * jnp.sqrt(times)[None, :] * outer)
    inner_drift = mean_rate * tau[None, :]
    inner_scale = vol[:, None] * jnp.sqrt(tau)[None, :]

    def one_path(carry, noise):
        totals, moments = carry
        shock = noise.astype(jnp.float32)
        level = outer_state * jnp.exp(inner_drift + inner_scale * shock)
        payoff = lax.optimization_barrier(jnp.min(level, axis=0))
        return ((totals + payoff, moments + payoff[None, :] * shock), None)
    init = (jnp.zeros((M,), jnp.float32), jnp.zeros((D, M), jnp.float32))
    (totals, moments), _ = lax.scan(one_path, init, inner_noise)
    point_value = totals / K
    point_grad = moments / (K * vol[:, None] * outer_state * jnp.sqrt(tau)[None, :])
    driver = driver_of(point_value)
    root_value = jnp.sum(totals) / (M * K) + jnp.sum(driver) / M
    terminal = lax.optimization_barrier(jnp.sum(jnp.sqrt(times)[None, :] * outer * totals[None, :] + jnp.sqrt(tau)[None, :] * moments, axis=1))
    integral = lax.optimization_barrier(jnp.sum(driver[None, :] * outer / jnp.sqrt(times)[None, :], axis=1))
    root_grad = terminal / (M * K * vol * start) + integral / (M * vol * start)
    return (jnp.reshape(root_value, (1,)), root_grad, point_value, point_grad)
```

```python
import functools

import jax
import jax.numpy as jnp
from jax import lax
from jax.experimental import pallas as pl
from jax.experimental.pallas import tpu as pltpu
from jax.sharding import PartitionSpec as P

drift = 0.02
delta = 2.0 / 3.0
rate_free = 0.02
gamma_high = 0.2
gamma_low = 0.02
value_high = 0.4
value_low = 0.7

NX, NY, NZ, NC = 4, 4, 8, 2
MESH = pl.DeviceIdType.MESH
F32 = jnp.float32
BF16 = jnp.bfloat16
CHUNKS = 5
PAIRS = (2, 1, 3, 0)


def driver_of(value):
    slope = jnp.clip((value - value_high) / (value_low - value_high), 0.0, 1.0)
    quota = gamma_high + (gamma_low - gamma_high) * slope
    return -(1.0 - delta) * quota * value - rate_free * value


def kernel(
    noise_hbm, outer_hbm, start_hbm, vol_hbm, times_hbm,
    rv_ref, rg_ref, pv_ref, pg_ref,
    noise, outer, start_v, vol_v, times_v,
    startp, volp, volb, abase, lmin, rx, pay, stage, nt, rc, ry, rz, scm, smy, smz, tot, dinv,
    in_sem, sx_s, sx_r, sc_s, sc_r, sy_s, sy_r, sz_s, sz_r, smc_s, smc_r, smy_s, smy_r, smz_s, smz_r,
):
    D, K, M = noise.shape
    path = lax.axis_index("path")
    x = lax.axis_index("dim")
    z = path // (NY * NC)
    y = (path // NC) % NY
    c = path % NC
    jz = z // 2

    def at_x(k):
        return (path, (x + k) % NX)

    def at(zz, yy, cc):
        return ((zz * NY + yy) * NC + cc, x)

    barrier = pltpu.get_barrier_semaphore()
    for k in range(1, NZ):
        pl.semaphore_signal(barrier, inc=1, device_id=at((z + k) % NZ, y, c), device_id_type=MESH)
    for k in range(1, NY):
        pl.semaphore_signal(barrier, inc=1, device_id=at(z, (y + k) % NY, c), device_id_type=MESH)
    for k in range(1, NX):
        pl.semaphore_signal(barrier, inc=1, device_id=at_x(k), device_id_type=MESH)
    pl.semaphore_signal(barrier, inc=1, device_id=at(z, y, 1 - c), device_id_type=MESH)

    small_in = [
        pltpu.make_async_copy(vol_hbm, vol_v, in_sem.at[0]),
        pltpu.make_async_copy(start_hbm, start_v, in_sem.at[1]),
        pltpu.make_async_copy(times_hbm, times_v, in_sem.at[2]),
        pltpu.make_async_copy(outer_hbm, outer, in_sem.at[3]),
    ]
    for cp in small_in:
        cp.start()
    per = D // CHUNKS
    noise_in = [
        pltpu.make_async_copy(
            noise_hbm.at[pl.ds(q * per, per)], noise.at[pl.ds(q * per, per)], in_sem.at[4 + q]
        )
        for q in range(CHUNKS)
    ]
    for cp in noise_in:
        cp.start()
    for cp in small_in:
        cp.wait()

    startp[...] = jnp.ones_like(startp)
    volp[...] = jnp.ones_like(volp)
    startp[:, 0:D] = start_v[...]
    volp[:, 0:D] = vol_v[...]
    vol = volp[...]
    begin = startp[...]
    times = times_v[...]
    tau = 1.0 - times
    root_t = jnp.sqrt(times)
    root_tau = jnp.sqrt(tau)
    inv_root_tau = 1.0 / root_tau
    offset = jnp.log(begin) + (drift - 0.5 * vol * vol)
    for h in range(2):
        volb[h * 128 : (h + 1) * 128, :] = jnp.broadcast_to(
            vol[:, h * 128 : (h + 1) * 128], (128, 128)
        ).T
        stage[h * 128 : (h + 1) * 128, :] = jnp.broadcast_to(
            offset[:, h * 128 : (h + 1) * 128], (128, 128)
        ).T
    for lo in range(0, D, 16):
        hi = min(lo + 16, D)
        for j in range(4):
            ls = slice(j * 128, (j + 1) * 128)
            o = outer[lo:hi, ls].astype(F32)
            abase[j, lo:hi, :] = (
                stage[lo:hi, :] + volb[lo:hi, :] * (root_t[:, ls] * o)
            ) * inv_root_tau[:, ls]

    acc = tuple(jnp.full((K, 128), 3.0e38, F32) for _ in range(4))
    unroll = 10
    for q in range(CHUNKS):
        noise_in[q].wait()

        def body(g, acc, q=q):
            acc = list(acc)
            for u in range(unroll):
                d = q * per + g * unroll + u
                v = volb[pl.ds(d, K, stride=0), :]
                for j in range(4):
                    n = noise[d, :, j * 128 : (j + 1) * 128].astype(F32)
                    a = abase[j, pl.ds(d, K, stride=0), :]
                    acc[j] = jnp.minimum(acc[j], n * v + a)
            return tuple(acc)

        acc = lax.fori_loop(0, per // unroll, body, acc)
    for j in range(4):
        lmin[:, j * 128 : (j + 1) * 128] = acc[j]

    pl.semaphore_wait(barrier, (NZ - 1) + (NY - 1) + (NX - 1) + 1)

    x_copies = []
    for k in (2, 1, 3):
        cp = pltpu.make_async_remote_copy(
            src_ref=lmin, dst_ref=rx.at[k - 1], send_sem=sx_s.at[k - 1], recv_sem=sx_r.at[k - 1],
            device_id=at_x(k), device_id_type=MESH,
        )
        cp.start()
        x_copies.append(cp)

    lane = lax.broadcasted_iota(jnp.int32, (K, M), 1)
    row = lax.broadcasted_iota(jnp.int32, (K, M), 0)
    pick = lane == path * K + row
    own_t = jnp.sum(jnp.where(pick, times, 0.0), axis=1, keepdims=True)
    own_outer = lax.dot_general(
        jnp.where(pick, 1.0, 0.0).astype(BF16), outer[...], (((1,), (1,)), ((), ())),
        preferred_element_type=F32,
    )
    vol_d = vol_v[...]
    own_state = start_v[...] * jnp.exp(
        (drift - 0.5 * vol_d * vol_d) * own_t + vol_d * jnp.sqrt(own_t) * own_outer
    )
    dinv[...] = 1.0 / ((K * NZ * NY * NC) * vol_d * own_state * (1.0 - own_t))

    for cp in x_copies:
        cp.wait_recv()
    least = jnp.minimum(jnp.minimum(lmin[...], rx[0]), jnp.minimum(rx[1], rx[2]))
    payoff = jnp.exp(root_tau * least)
    pay[...] = payoff * root_tau
    totals = jnp.sum(payoff, axis=0, keepdims=True)

    sub = lax.broadcasted_iota(jnp.int32, (8, 128), 0)
    bit2 = (sub & 4) == 0
    bit1 = (sub & 2) == 0
    bit0 = (sub & 1) == 0

    def merge(a, b, first, shift):
        if shift == 4:
            return jnp.where(first, a, b) + pltpu.roll(jnp.where(first, b, a), 4, axis=0)
        return jnp.where(
            first,
            a + pltpu.roll(a, 8 - shift, axis=0),
            b + pltpu.roll(b, shift, axis=0),
        )

    def sums_of(ys):
        c4 = [merge(ys[s], ys[s + 4], bit2, 4) for s in range(4)]
        e2 = [merge(c4[s], c4[s + 2], bit1, 2) for s in range(2)]
        return merge(e2[0], e2[1], bit0, 1)

    def core_copy(t):
        return pltpu.make_async_remote_copy(
            src_ref=nt.at[t, 1 - c], dst_ref=rc.at[t], send_sem=sc_s.at[t], recv_sem=sc_r.at[t],
            device_id=at(z, y, 1 - c), device_id_type=MESH,
        )

    def y_copy(t, k):
        peer = (y + k) % NY
        return pltpu.make_async_remote_copy(
            src_ref=nt.at[t, c, peer], dst_ref=ry.at[t, k - 1],
            send_sem=sy_s.at[t * 3 + k - 1], recv_sem=sy_r.at[t * 3 + k - 1],
            device_id=at(z, peer, c), device_id_type=MESH,
        )

    def after_core(t):
        core_copy(t).wait_recv()
        nt[t, c] = nt[t, c] + rc[t]
        for k in (2, 1, 3):
            y_copy(t, k).start()

    wsum = jnp.zeros((8, 256), F32)
    full = D // 8
    for t, off in enumerate(PAIRS):
        j = (jz + off) % 4
        lanes = pl.ds(pl.multiple_of(j * 128, 128), 128)
        p = pay[:, lanes]

        def group(g, _, p=p, lanes=lanes):
            ys = [noise[g * 8 + s, :, lanes].astype(F32) * p for s in range(8)]
            stage[pl.ds(pl.multiple_of(g * 8, 8), 8), :] = sums_of(ys)
            return 0

        lax.fori_loop(0, full, group, 0)
        rest = [noise[full * 8 + s, :, lanes].astype(F32) * p for s in range(D - full * 8)]
        rest += [jnp.zeros((8, 128), F32)] * (8 - len(rest))
        stage[full * 8 : full * 8 + 8, :] = sums_of(rest)
        for h in range(2):
            block = stage[h * 128 : (h + 1) * 128, :].T
            part = jnp.zeros((8, 128), F32)
            for q in range(16):
                zz, yy, cc = q // 8, (q // 2) % 4, q % 2
                piece = block[q * 8 : (q + 1) * 8, :]
                nt[t, cc, yy, zz, :, h * 128 : (h + 1) * 128] = piece
                part = part + piece
            wsum = wsum + (
                jnp.concatenate([part, jnp.zeros((8, 128), F32)], axis=1)
                if h == 0
                else jnp.concatenate([jnp.zeros((8, 128), F32), part], axis=1)
            )
        if t == 3:
            w = jnp.sum(wsum, axis=0, keepdims=True)
            scm[0] = jnp.concatenate(
                [totals[:, k * 128 : (k + 1) * 128] for k in range(4)]
                + [w[:, 0:128], w[:, 128:256], jnp.zeros((2, 128), F32)],
                axis=0,
            )
            small_core = pltpu.make_async_remote_copy(
                src_ref=scm.at[0], dst_ref=scm.at[1], send_sem=smc_s, recv_sem=smc_r,
                device_id=at(z, y, 1 - c), device_id_type=MESH,
            )
            small_core.start()
        core_copy(t).start()
        if t >= 1:
            after_core(t - 1)

    small_core.wait_recv()
    smy[y] = scm[0] + scm[1]
    small_y = []
    for k in (2, 1, 3):
        cp = pltpu.make_async_remote_copy(
            src_ref=smy.at[y], dst_ref=smy.at[y], send_sem=smy_s.at[k - 1], recv_sem=smy_r.at[k - 1],
            device_id=at(z, (y + k) % NY, c), device_id_type=MESH,
        )
        cp.start()
        small_y.append(cp)
    after_core(3)

    def z_copy(t, peer, zz):
        return pltpu.make_async_remote_copy(
            src_ref=nt.at[t, c, y, zz], dst_ref=rz.at[z], send_sem=sz_s.at[peer], recv_sem=sz_r.at[z],
            device_id=at(peer, y, c), device_id_type=MESH,
        )

    def after_y(t):
        for k in range(1, NY):
            y_copy(t, k).wait_recv()
        nt[t, c, y] = nt[t, c, y] + (ry[t, 0] + ry[t, 1] + ry[t, 2])
        base = 2 * ((jz + PAIRS[t]) % 4)
        if PAIRS[t] == 0:
            peer = base + 1 - z % 2
            z_copy(t, peer, 1 - z % 2).start()
        else:
            for zz in range(2):
                z_copy(t, base + zz, zz).start()

    after_y(0)
    for cp in small_y:
        cp.wait_recv()
    smz[z] = (smy[0] + smy[1]) + (smy[2] + smy[3])
    small_z = []
    for k in (4, 3, 5, 2, 6, 1, 7):
        cp = pltpu.make_async_remote_copy(
            src_ref=smz.at[z], dst_ref=smz.at[z], send_sem=smz_s.at[k - 1], recv_sem=smz_r.at[k - 1],
            device_id=at((z + k) % NZ, y, c), device_id_type=MESH,
        )
        cp.start()
        small_z.append(cp)
    after_y(1)
    after_y(2)
    after_y(3)

    for cp in small_z:
        cp.wait_recv()
    whole = ((smz[0] + smz[1]) + (smz[2] + smz[3])) + ((smz[4] + smz[5]) + (smz[6] + smz[7]))
    inner = K * NZ * NY * NC
    tot[...] = whole
    totals = jnp.concatenate([whole[k : k + 1, :] for k in range(4)], axis=1)
    driver = driver_of(totals * (1.0 / inner))
    rv_ref[...] = (
        jnp.sum(totals, axis=1, keepdims=True) * (1.0 / (M * inner))
        + jnp.sum(driver, axis=1, keepdims=True) * (1.0 / M)
    )
    weight = root_t * totals * (1.0 / (M * inner)) + driver / (root_t * M)
    w_hi = weight.astype(BF16).astype(F32)
    w_mid = (weight - w_hi).astype(BF16).astype(F32)
    w_lo = weight - w_hi - w_mid
    rows = lax.broadcasted_iota(jnp.int32, (8, M), 0)
    lhs = jnp.where(rows == 0, w_hi, jnp.where(rows == 1, w_mid, jnp.where(rows == 2, w_lo, 0.0)))
    prod = lax.dot_general(
        lhs.astype(BF16), outer[...], (((1,), (1,)), ((), ())), preferred_element_type=F32
    )
    noise_sum = jnp.sum(prod, axis=0, keepdims=True)
    moment_sum = jnp.concatenate([whole[4:5, :], whole[5:6, :]], axis=1)[:, 0:D]
    rg_ref[...] = (noise_sum + moment_sum * (1.0 / (M * inner))) / (vol_v[...] * start_v[...])
    own_row = tot[pl.ds(path // 16, 1), :] * (1.0 / inner)
    own_row = pltpu.roll(jnp.broadcast_to(own_row, (8, 128)), (128 - (path % 16) * 8) % 128, axis=1)
    pv_ref[...] = own_row[0:1, 0:8]

    own = nt[3, c, y, z % 2]
    for k in range(1, NZ):
        src = (z + k) % NZ
        pltpu.make_async_remote_copy(
            src_ref=rz.at[src], dst_ref=rz.at[src], send_sem=sz_s.at[src], recv_sem=sz_r.at[src],
            device_id=at(src, y, c), device_id_type=MESH,
        ).wait_recv()
        own = own + rz[src]
    pg_ref[...] = own[:, 0:D] * dinv[...]

    for cp in x_copies + small_y + small_z + [small_core]:
        cp.wait_send()
    for t in range(4):
        core_copy(t).wait_send()
        for k in range(1, NY):
            y_copy(t, k).wait_send()
    for k in range(1, NZ):
        peer = (z + k) % NZ
        pltpu.make_async_remote_copy(
            src_ref=rz.at[peer], dst_ref=rz.at[peer], send_sem=sz_s.at[peer], recv_sem=sz_r.at[peer],
            device_id=at(peer, y, c), device_id_type=MESH,
        ).wait_send()


def per_device(inner_noise, outer_noise, start, vol, times):
    K, D, M = inner_noise.shape
    hbm = pl.BlockSpec(memory_space=pltpu.HBM)
    vmem = pl.BlockSpec(memory_space=pltpu.VMEM)
    dma = pltpu.SemaphoreType.DMA
    V = pltpu.VMEM
    root_value, root_grad, point_value, point_grad = pl.pallas_call(
        kernel,
        out_shape=(
            jax.ShapeDtypeStruct((1, 1), F32),
            jax.ShapeDtypeStruct((1, D), F32),
            jax.ShapeDtypeStruct((1, 8), F32),
            jax.ShapeDtypeStruct((8, D), F32),
        ),
        in_specs=[hbm] * 5,
        out_specs=(vmem,) * 4,
        scratch_shapes=[
            V((D, K, M), BF16), V((D, M), BF16), V((1, D), F32), V((1, D), F32), V((1, M), F32),
            V((1, 256), F32), V((1, 256), F32), V((256, 128), F32), V((4, 256, 128), F32),
            V((K, M), F32), V((3, K, M), F32), V((K, M), F32), V((256, 128), F32),
            V((4, NC, NY, 2, 8, 256), F32), V((4, NY, 2, 8, 256), F32),
            V((4, 3, 2, 8, 256), F32), V((NZ, 8, 256), F32),
            V((2, 8, 128), F32), V((NY, 8, 128), F32), V((NZ, 8, 128), F32), V((8, 128), F32),
            V((8, D), F32),
            dma((4 + CHUNKS,)), dma((3,)), dma((3,)), dma((4,)), dma((4,)), dma((12,)), dma((12,)),
            dma((NZ,)), dma((NZ,)), dma, dma, dma((3,)), dma((3,)), dma((7,)), dma((7,)),
        ],
        compiler_params=pltpu.CompilerParams(
            collective_id=0, has_side_effects=True, vmem_limit_bytes=32 * 1024 * 1024
        ),
    )(
        jnp.transpose(inner_noise, (1, 0, 2)), outer_noise, start[None], vol[None], times[None]
    )
    return root_value[0], root_grad[0], point_value[0], point_grad.T


def solution(mesh):
    in_specs = (P("path", "dim", None), P("dim", None), P("dim"), P("dim"), P())
    out_specs = (P(), P("dim"), P("path"), P("dim", "path"))
    return jax.shard_map(
        per_device, mesh=mesh, in_specs=in_specs, out_specs=out_specs, check_vma=False
    )
```

```python
import functools

import jax
import jax.numpy as jnp
from jax import lax
from jax.experimental import pallas as pl
from jax.experimental.pallas import tpu as pltpu
from jax.sharding import PartitionSpec as P

drift = 0.02
delta = 2.0 / 3.0
rate_free = 0.02
gamma_high = 0.2
gamma_low = 0.02
value_high = 0.4
value_low = 0.7

NX, NY, NZ, NC = 4, 4, 8, 2
MESH = pl.DeviceIdType.MESH
F32 = jnp.float32
BF16 = jnp.bfloat16
CHUNKS = 5
PAIRS = (2, 1, 3, 0)


def driver_of(value):
    slope = jnp.clip((value - value_high) / (value_low - value_high), 0.0, 1.0)
    quota = gamma_high + (gamma_low - gamma_high) * slope
    return -(1.0 - delta) * quota * value - rate_free * value


def kernel(
    noise_hbm, outer_hbm, start_hbm, vol_hbm, times_hbm,
    rv_ref, rg_ref, pv_ref, pg_ref,
    noise, outer, start_v, vol_v, times_v,
    startp, volp, volb, abase, lmin, rx, pay, stage, nt, rc, ry, rz, scm, smy, smz, tot, dinv,
    in_sem, sx_s, sx_r, sc_s, sc_r, sy_s, sy_r, sz_s, sz_r, smc_s, smc_r, smy_s, smy_r, smz_s, smz_r,
):
    D, K, M = noise.shape
    path = lax.axis_index("path")
    x = lax.axis_index("dim")
    z = path // (NY * NC)
    y = (path // NC) % NY
    c = path % NC
    jz = z // 2

    def at_x(k):
        return (path, (x + k) % NX)

    def at(zz, yy, cc):
        return ((zz * NY + yy) * NC + cc, x)

    barrier = pltpu.get_barrier_semaphore()
    for k in range(1, NZ):
        pl.semaphore_signal(barrier, inc=1, device_id=at((z + k) % NZ, y, c), device_id_type=MESH)
    for k in range(1, NY):
        pl.semaphore_signal(barrier, inc=1, device_id=at(z, (y + k) % NY, c), device_id_type=MESH)
    for k in range(1, NX):
        pl.semaphore_signal(barrier, inc=1, device_id=at_x(k), device_id_type=MESH)
    pl.semaphore_signal(barrier, inc=1, device_id=at(z, y, 1 - c), device_id_type=MESH)

    small_in = [
        pltpu.make_async_copy(vol_hbm, vol_v, in_sem.at[0]),
        pltpu.make_async_copy(start_hbm, start_v, in_sem.at[1]),
        pltpu.make_async_copy(times_hbm, times_v, in_sem.at[2]),
        pltpu.make_async_copy(outer_hbm, outer, in_sem.at[3]),
    ]
    for cp in small_in:
        cp.start()
    per = D // CHUNKS
    noise_in = [
        pltpu.make_async_copy(
            noise_hbm.at[pl.ds(q * per, per)], noise.at[pl.ds(q * per, per)], in_sem.at[4 + q]
        )
        for q in range(CHUNKS)
    ]
    for cp in noise_in:
        cp.start()
    for cp in small_in:
        cp.wait()

    startp[...] = jnp.ones_like(startp)
    volp[...] = jnp.ones_like(volp)
    startp[:, 0:D] = start_v[...]
    volp[:, 0:D] = vol_v[...]
    vol = volp[...]
    begin = startp[...]
    times = times_v[...]
    tau = 1.0 - times
    root_t = jnp.sqrt(times)
    root_tau = jnp.sqrt(tau)
    inv_root_tau = 1.0 / root_tau
    offset = jnp.log(begin) + (drift - 0.5 * vol * vol)
    for h in range(2):
        volb[h * 128 : (h + 1) * 128, :] = jnp.broadcast_to(
            vol[:, h * 128 : (h + 1) * 128], (128, 128)
        ).T
        stage[h * 128 : (h + 1) * 128, :] = jnp.broadcast_to(
            offset[:, h * 128 : (h + 1) * 128], (128, 128)
        ).T
    for lo in range(0, D, 16):
        hi = min(lo + 16, D)
        for j in range(4):
            ls = slice(j * 128, (j + 1) * 128)
            o = outer[lo:hi, ls].astype(F32)
            abase[j, lo:hi, :] = (
                stage[lo:hi, :] + volb[lo:hi, :] * (root_t[:, ls] * o)
            ) * inv_root_tau[:, ls]

    acc = tuple(jnp.full((K, 128), 3.0e38, F32) for _ in range(4))
    unroll = 10
    for q in range(CHUNKS):
        noise_in[q].wait()

        def body(g, acc, q=q):
            acc = list(acc)
            for u in range(unroll):
                d = q * per + g * unroll + u
                v = volb[pl.ds(d, K, stride=0), :]
                for j in range(4):
                    n = noise[d, :, j * 128 : (j + 1) * 128].astype(F32)
                    a = abase[j, pl.ds(d, K, stride=0), :]
                    acc[j] = jnp.minimum(acc[j], n * v + a)
            return tuple(acc)

        acc = lax.fori_loop(0, per // unroll, body, acc)
    for j in range(4):
        lmin[:, j * 128 : (j + 1) * 128] = acc[j]

    pl.semaphore_wait(barrier, (NZ - 1) + (NY - 1) + (NX - 1) + 1)

    x_copies = []
    for k in (2, 1, 3):
        cp = pltpu.make_async_remote_copy(
            src_ref=lmin, dst_ref=rx.at[k - 1], send_sem=sx_s.at[k - 1], recv_sem=sx_r.at[k - 1],
            device_id=at_x(k), device_id_type=MESH,
        )
        cp.start()
        x_copies.append(cp)

    lane = lax.broadcasted_iota(jnp.int32, (K, M), 1)
    row = lax.broadcasted_iota(jnp.int32, (K, M), 0)
    pick = lane == path * K + row
    own_t = jnp.sum(jnp.where(pick, times, 0.0), axis=1, keepdims=True)
    own_outer = lax.dot_general(
        jnp.where(pick, 1.0, 0.0).astype(BF16), outer[...], (((1,), (1,)), ((), ())),
        preferred_element_type=F32,
    )
    vol_d = vol_v[...]
    own_state = start_v[...] * jnp.exp(
        (drift - 0.5 * vol_d * vol_d) * own_t + vol_d * jnp.sqrt(own_t) * own_outer
    )
    dinv[...] = 1.0 / ((K * NZ * NY * NC) * vol_d * own_state * (1.0 - own_t))

    for cp in x_copies:
        cp.wait_recv()
    least = jnp.minimum(jnp.minimum(lmin[...], rx[0]), jnp.minimum(rx[1], rx[2]))
    payoff = jnp.exp(root_tau * least)
    pay[...] = payoff * root_tau
    totals = jnp.sum(payoff, axis=0, keepdims=True)

    sub = lax.broadcasted_iota(jnp.int32, (8, 128), 0)
    bit2 = (sub & 4) == 0
    bit1 = (sub & 2) == 0
    bit0 = (sub & 1) == 0

    def merge(a, b, first, shift):
        if shift == 4:
            return jnp.where(first, a, b) + pltpu.roll(jnp.where(first, b, a), 4, axis=0)
        return jnp.where(
            first,
            a + pltpu.roll(a, 8 - shift, axis=0),
            b + pltpu.roll(b, shift, axis=0),
        )

    def sums_of(ys):
        c4 = [merge(ys[s], ys[s + 4], bit2, 4) for s in range(4)]
        e2 = [merge(c4[s], c4[s + 2], bit1, 2) for s in range(2)]
        return merge(e2[0], e2[1], bit0, 1)

    def core_copy(t):
        return pltpu.make_async_remote_copy(
            src_ref=nt.at[t, 1 - c], dst_ref=rc.at[t], send_sem=sc_s.at[t], recv_sem=sc_r.at[t],
            device_id=at(z, y, 1 - c), device_id_type=MESH,
        )

    def y_copy(t, k):
        peer = (y + k) % NY
        return pltpu.make_async_remote_copy(
            src_ref=nt.at[t, c, peer], dst_ref=ry.at[t, k - 1],
            send_sem=sy_s.at[t * 3 + k - 1], recv_sem=sy_r.at[t * 3 + k - 1],
            device_id=at(z, peer, c), device_id_type=MESH,
        )

    def after_core(t):
        core_copy(t).wait_recv()
        nt[t, c] = nt[t, c] + rc[t]
        for k in (2, 1, 3):
            y_copy(t, k).start()

    wsum = jnp.zeros((8, 256), F32)
    full = D // 8
    for t, off in enumerate(PAIRS):
        j = (jz + off) % 4
        lanes = pl.ds(pl.multiple_of(j * 128, 128), 128)
        p = pay[:, lanes]

        def group(g, _, p=p, lanes=lanes):
            ys = [noise[g * 8 + s, :, lanes].astype(F32) * p for s in range(8)]
            stage[pl.ds(pl.multiple_of(g * 8, 8), 8), :] = sums_of(ys)
            return 0

        lax.fori_loop(0, full, group, 0)
        rest = [noise[full * 8 + s, :, lanes].astype(F32) * p for s in range(D - full * 8)]
        rest += [jnp.zeros((8, 128), F32)] * (8 - len(rest))
        stage[full * 8 : full * 8 + 8, :] = sums_of(rest)
        for h in range(2):
            block = stage[h * 128 : (h + 1) * 128, :].T
            part = jnp.zeros((8, 128), F32)
            for q in range(16):
                zz, yy, cc = q // 8, (q // 2) % 4, q % 2
                piece = block[q * 8 : (q + 1) * 8, :]
                nt[t, cc, yy, zz, :, h * 128 : (h + 1) * 128] = piece
                part = part + piece
            wsum = wsum + (
                jnp.concatenate([part, jnp.zeros((8, 128), F32)], axis=1)
                if h == 0
                else jnp.concatenate([jnp.zeros((8, 128), F32), part], axis=1)
            )
        if t == 3:
            w = jnp.sum(wsum, axis=0, keepdims=True)
            scm[0] = jnp.concatenate(
                [totals[:, k * 128 : (k + 1) * 128] for k in range(4)]
                + [w[:, 0:128], w[:, 128:256], jnp.zeros((2, 128), F32)],
                axis=0,
            )
            small_core = pltpu.make_async_remote_copy(
                src_ref=scm.at[0], dst_ref=scm.at[1], send_sem=smc_s, recv_sem=smc_r,
                device_id=at(z, y, 1 - c), device_id_type=MESH,
            )
            small_core.start()
        core_copy(t).start()
        if t >= 1:
            after_core(t - 1)

    small_core.wait_recv()
    smy[y] = scm[0] + scm[1]
    small_y = []
    for k in (2, 1, 3):
        cp = pltpu.make_async_remote_copy(
            src_ref=smy.at[y], dst_ref=smy.at[y], send_sem=smy_s.at[k - 1], recv_sem=smy_r.at[k - 1],
            device_id=at(z, (y + k) % NY, c), device_id_type=MESH,
        )
        cp.start()
        small_y.append(cp)
    after_core(3)

    def z_copy(t, peer, zz):
        return pltpu.make_async_remote_copy(
            src_ref=nt.at[t, c, y, zz], dst_ref=rz.at[z], send_sem=sz_s.at[peer], recv_sem=sz_r.at[z],
            device_id=at(peer, y, c), device_id_type=MESH,
        )

    def after_y(t):
        for k in range(1, NY):
            y_copy(t, k).wait_recv()
        nt[t, c, y] = nt[t, c, y] + (ry[t, 0] + ry[t, 1] + ry[t, 2])
        base = 2 * ((jz + PAIRS[t]) % 4)
        if PAIRS[t] == 0:
            peer = base + 1 - z % 2
            z_copy(t, peer, 1 - z % 2).start()
        else:
            for zz in range(2):
                z_copy(t, base + zz, zz).start()

    after_y(0)
    for cp in small_y:
        cp.wait_recv()
    smz[z] = (smy[0] + smy[1]) + (smy[2] + smy[3])
    small_z = []
    for k in (4, 3, 5, 2, 6, 1, 7):
        cp = pltpu.make_async_remote_copy(
            src_ref=smz.at[z], dst_ref=smz.at[z], send_sem=smz_s.at[k - 1], recv_sem=smz_r.at[k - 1],
            device_id=at((z + k) % NZ, y, c), device_id_type=MESH,
        )
        cp.start()
        small_z.append(cp)
    after_y(1)
    after_y(2)
    after_y(3)

    for cp in small_z:
        cp.wait_recv()
    whole = ((smz[0] + smz[1]) + (smz[2] + smz[3])) + ((smz[4] + smz[5]) + (smz[6] + smz[7]))
    inner = K * NZ * NY * NC
    tot[...] = whole
    totals = jnp.concatenate([whole[k : k + 1, :] for k in range(4)], axis=1)
    driver = driver_of(totals * (1.0 / inner))
    rv_ref[...] = jnp.zeros((1, 128), F32) + (
        jnp.sum(totals, axis=1, keepdims=True) * (1.0 / (M * inner))
        + jnp.sum(driver, axis=1, keepdims=True) * (1.0 / M)
    )
    weight = root_t * totals * (1.0 / (M * inner)) + driver / (root_t * M)
    w_hi = weight.astype(BF16).astype(F32)
    w_mid = (weight - w_hi).astype(BF16).astype(F32)
    w_lo = weight - w_hi - w_mid
    rows = lax.broadcasted_iota(jnp.int32, (8, M), 0)
    lhs = jnp.where(rows == 0, w_hi, jnp.where(rows == 1, w_mid, jnp.where(rows == 2, w_lo, 0.0)))
    prod = lax.dot_general(
        lhs.astype(BF16), outer[...], (((1,), (1,)), ((), ())), preferred_element_type=F32
    )
    noise_sum = jnp.sum(prod, axis=0, keepdims=True)
    moment_sum = jnp.concatenate([whole[4:5, :], whole[5:6, :]], axis=1)[:, 0:D]
    rg_ref[...] = (noise_sum + moment_sum * (1.0 / (M * inner))) / (vol_v[...] * start_v[...])
    own_row = tot[pl.ds(path // 16, 1), :] * (1.0 / inner)
    own_row = pltpu.roll(jnp.broadcast_to(own_row, (8, 128)), (128 - (path % 16) * 8) % 128, axis=1)
    pv_ref[...] = own_row[0:1, 0:8]

    own = nt[3, c, y, z % 2]
    for k in range(1, NZ):
        src = (z + k) % NZ
        pltpu.make_async_remote_copy(
            src_ref=rz.at[src], dst_ref=rz.at[src], send_sem=sz_s.at[src], recv_sem=sz_r.at[src],
            device_id=at(src, y, c), device_id_type=MESH,
        ).wait_recv()
        own = own + rz[src]
    pg_ref[...] = own[:, 0:D] * dinv[...]

    for cp in x_copies + small_y + small_z + [small_core]:
        cp.wait_send()
    for t in range(4):
        core_copy(t).wait_send()
        for k in range(1, NY):
            y_copy(t, k).wait_send()
    for k in range(1, NZ):
        peer = (z + k) % NZ
        pltpu.make_async_remote_copy(
            src_ref=rz.at[peer], dst_ref=rz.at[peer], send_sem=sz_s.at[peer], recv_sem=sz_r.at[peer],
            device_id=at(peer, y, c), device_id_type=MESH,
        ).wait_send()


def hand_out(a, b, c, d, a_out, b_out, c_out, d_out, one, sem):
    one[...] = a[0:1, 0:1]
    pairs = ((d, d_out), (b, b_out), (c, c_out), (one, a_out))
    copies = [pltpu.make_async_copy(src, dst, sem.at[k]) for k, (src, dst) in enumerate(pairs)]
    for cp in copies:
        cp.start()
    for cp in copies:
        cp.wait()


def per_device(inner_noise, outer_noise, start, vol, times):
    K, D, M = inner_noise.shape
    hbm = pl.BlockSpec(memory_space=pltpu.HBM)
    vmem = pl.BlockSpec(memory_space=pltpu.VMEM)
    dma = pltpu.SemaphoreType.DMA
    V = pltpu.VMEM
    results = pl.pallas_call(
        kernel,
        out_shape=(V((1, 128), F32), V((1, D), F32), V((1, 8), F32), V((8, D), F32)),
        in_specs=[hbm] * 5,
        out_specs=(vmem,) * 4,
        scratch_shapes=[
            V((D, K, M), BF16), V((D, M), BF16), V((1, D), F32), V((1, D), F32), V((1, M), F32),
            V((1, 256), F32), V((1, 256), F32), V((256, 128), F32), V((4, 256, 128), F32),
            V((K, M), F32), V((3, K, M), F32), V((K, M), F32), V((256, 128), F32),
            V((4, NC, NY, 2, 8, 256), F32), V((4, NY, 2, 8, 256), F32),
            V((4, 3, 2, 8, 256), F32), V((NZ, 8, 256), F32),
            V((2, 8, 128), F32), V((NY, 8, 128), F32), V((NZ, 8, 128), F32), V((8, 128), F32),
            V((8, D), F32),
            dma((4 + CHUNKS,)), dma((3,)), dma((3,)), dma((4,)), dma((4,)), dma((12,)), dma((12,)),
            dma((NZ,)), dma((NZ,)), dma, dma, dma((3,)), dma((3,)), dma((7,)), dma((7,)),
        ],
        compiler_params=pltpu.CompilerParams(
            collective_id=0, has_side_effects=True
        ),
    )(
        jnp.transpose(inner_noise, (1, 0, 2)), outer_noise, start[None], vol[None], times[None]
    )
    root_value, root_grad, point_value, point_grad = pl.pallas_call(
        hand_out,
        out_shape=tuple(jax.ShapeDtypeStruct(s, F32) for s in ((1, 1), (1, D), (1, 8), (8, D))),
        in_specs=[vmem] * 4,
        out_specs=(hbm,) * 4,
        scratch_shapes=[V((1, 1), F32), dma((4,))],
        compiler_params=pltpu.CompilerParams(vmem_limit_bytes=1024 * 1024),
    )(*results)
    return root_value[0], root_grad[0], point_value[0], point_grad.T


def solution(mesh):
    in_specs = (P("path", "dim", None), P("dim", None), P("dim"), P("dim"), P())
    out_specs = (P(), P("dim"), P("path"), P("dim", "path"))
    return jax.shard_map(
        per_device, mesh=mesh, in_specs=in_specs, out_specs=out_specs, check_vma=False
    )
```

```python
import functools

import jax
import jax.numpy as jnp
from jax import lax
from jax.experimental import pallas as pl
from jax.experimental.pallas import tpu as pltpu
from jax.sharding import PartitionSpec as P

drift = 0.02
delta = 2.0 / 3.0
rate_free = 0.02
gamma_high = 0.2
gamma_low = 0.02
value_high = 0.4
value_low = 0.7

NX, NY, NZ, NC = 4, 4, 8, 2
MESH = pl.DeviceIdType.MESH
F32 = jnp.float32
BF16 = jnp.bfloat16
PAIRS = (2, 1, 3, 0)


def driver_of(value):
    slope = jnp.clip((value - value_high) / (value_low - value_high), 0.0, 1.0)
    quota = gamma_high + (gamma_low - gamma_high) * slope
    return -(1.0 - delta) * quota * value - rate_free * value


def kernel(
    noise_hbm, outer_hbm, start_hbm, vol_hbm, times_hbm,
    rv_ref, rg_ref, pv_ref, pg_ref,
    noise, outer, start_v, vol_v, times_v,
    startp, volp, volb, abase, lmin, rx, rtau, stage, nt, rc, ry, rz, smy, smz, tot, dinv,
    in_sem, sx_s, sx_r, sc_s, sc_r, sy_s, sy_r, sz_s, sz_r, smy_s, smy_r, smz_s, smz_r, know,
):
    D, K, M = noise_hbm.shape
    path = lax.axis_index("path")
    x = lax.axis_index("dim")
    z = path // (NY * NC)
    y = (path // NC) % NY
    c = path % NC
    jz = z // 2

    def at_x(k):
        return (path, (x + k) % NX)

    def at(zz, yy, cc):
        return ((zz * NY + yy) * NC + cc, x)

    barrier = pltpu.get_barrier_semaphore()
    near = [at((z + k) % NZ, y, c) for k in (1, NZ - 1)]
    near += [at(z, (y + k) % NY, cc) for k in (1, NY - 1) for cc in (c, 1 - c)]
    near += [at_x(k) for k in (1, 2, 3)] + [at(z, y, 1 - c)]
    for peer in near:
        pl.semaphore_signal(barrier, inc=1, device_id=peer, device_id_type=MESH)

    def tell(sem, peer):
        pl.semaphore_signal(sem, inc=1, device_id=peer, device_id_type=MESH)

    z_next, z_last = at((z + 1) % NZ, y, c), at((z + NZ - 1) % NZ, y, c)

    small_in = [
        pltpu.make_async_copy(vol_hbm, vol_v, in_sem.at[0]),
        pltpu.make_async_copy(start_hbm, start_v, in_sem.at[1]),
        pltpu.make_async_copy(times_hbm, times_v, in_sem.at[2]),
        pltpu.make_async_copy(outer_hbm, outer, in_sem.at[3]),
    ]
    for cp in small_in:
        cp.start()
    blocks = [(jz + off) % 4 for off in PAIRS]
    noise_in = [
        pltpu.make_async_copy(
            noise_hbm.at[:, :, pl.ds(pl.multiple_of(j * 128, 128), 128)], noise.at[t], in_sem.at[4 + t]
        )
        for t, j in enumerate(blocks)
    ]
    for cp in noise_in:
        cp.start()
    for cp in small_in:
        cp.wait()

    startp[...] = jnp.ones_like(startp)
    volp[...] = jnp.ones_like(volp)
    startp[:, 0:D] = start_v[...]
    volp[:, 0:D] = vol_v[...]
    vol = volp[...]
    begin = startp[...]
    times = times_v[...]
    tau = 1.0 - times
    root_t = jnp.sqrt(times)
    root_tau = jnp.sqrt(tau)
    inv_root_tau = 1.0 / root_tau
    offset = jnp.log(begin) + (drift - 0.5 * vol * vol)
    for h in range(2):
        volb[h * 128 : (h + 1) * 128, :] = jnp.broadcast_to(
            vol[:, h * 128 : (h + 1) * 128], (128, 128)
        ).T
        stage[h * 128 : (h + 1) * 128, :] = jnp.broadcast_to(
            offset[:, h * 128 : (h + 1) * 128], (128, 128)
        ).T
    for lo in range(0, D, 16):
        hi = min(lo + 16, D)
        for j in range(4):
            ls = slice(j * 128, (j + 1) * 128)
            o = outer[lo:hi, ls].astype(F32)
            abase[j, lo:hi, :] = (
                stage[lo:hi, :] + volb[lo:hi, :] * (root_t[:, ls] * o)
            ) * inv_root_tau[:, ls]

    def x_copy(t, k):
        return pltpu.make_async_remote_copy(
            src_ref=lmin.at[t], dst_ref=rx.at[k - 1, t],
            send_sem=sx_s.at[t * 3 + k - 1], recv_sem=sx_r.at[t * 3 + k - 1],
            device_id=at_x(k), device_id_type=MESH,
        )

    unroll = 10
    for t, j in enumerate(blocks):
        noise_in[t].wait()

        def body(g, acc, t=t, j=j):
            terms = []
            for u in range(unroll):
                d = g * unroll + u
                n = noise[t, d].astype(F32)
                terms.append(
                    n * volb[pl.ds(d, K, stride=0), :] + abase[j, pl.ds(d, K, stride=0), :]
                )
            while len(terms) > 1:
                pairs = [jnp.minimum(a, b) for a, b in zip(terms[::2], terms[1::2])]
                terms = pairs + terms[len(pairs) * 2 :]
            return jnp.minimum(acc, terms[0])

        lmin[t] = lax.fori_loop(0, D // unroll, body, jnp.full((K, 128), 3.0e38, F32))
        if t == 0:
            pl.semaphore_wait(barrier, len(near))
            tell(know.at[0], at(z, (y + NY - 1) % NY, c))
            tell(know.at[1], z_last)
            tell(know.at[2], z_next)
        for k in (2, 1, 3):
            x_copy(t, k).start()

    lane = lax.broadcasted_iota(jnp.int32, (K, M), 1)
    row = lax.broadcasted_iota(jnp.int32, (K, M), 0)
    pick = lane == path * K + row
    own_t = jnp.sum(jnp.where(pick, times, 0.0), axis=1, keepdims=True)
    own_outer = lax.dot_general(
        jnp.where(pick, 1.0, 0.0).astype(BF16), outer[...], (((1,), (1,)), ((), ())),
        preferred_element_type=F32,
    )
    vol_d = vol_v[...]
    own_state = start_v[...] * jnp.exp(
        (drift - 0.5 * vol_d * vol_d) * own_t + vol_d * jnp.sqrt(own_t) * own_outer
    )
    dinv[...] = 1.0 / ((K * NZ * NY * NC) * vol_d * own_state * (1.0 - own_t))

    rtau[...] = root_tau

    sub = lax.broadcasted_iota(jnp.int32, (8, 128), 0)
    bit2 = (sub & 4) == 0
    bit1 = (sub & 2) == 0
    bit0 = (sub & 1) == 0

    def merge(a, b, first, shift):
        if shift == 4:
            return jnp.where(first, a, b) + pltpu.roll(jnp.where(first, b, a), 4, axis=0)
        return jnp.where(
            first,
            a + pltpu.roll(a, 8 - shift, axis=0),
            b + pltpu.roll(b, shift, axis=0),
        )

    def sums_of(ys):
        c4 = [merge(ys[s], ys[s + 4], bit2, 4) for s in range(4)]
        e2 = [merge(c4[s], c4[s + 2], bit1, 2) for s in range(2)]
        return merge(e2[0], e2[1], bit0, 1)

    pl.semaphore_wait(know.at[0], 1)
    pl.semaphore_wait(know.at[1], 1)
    pl.semaphore_wait(know.at[2], 1)
    tell(know.at[3], z_last)
    tell(know.at[4], z_next)

    def core_copy(t):
        return pltpu.make_async_remote_copy(
            src_ref=nt.at[t, 1 - c], dst_ref=rc.at[t], send_sem=sc_s.at[t], recv_sem=sc_r.at[t],
            device_id=at(z, y, 1 - c), device_id_type=MESH,
        )

    def y_copy(t, k):
        peer = (y + k) % NY
        return pltpu.make_async_remote_copy(
            src_ref=nt.at[t, c, peer], dst_ref=ry.at[t, k - 1],
            send_sem=sy_s.at[t * 3 + k - 1], recv_sem=sy_r.at[t * 3 + k - 1],
            device_id=at(z, peer, c), device_id_type=MESH,
        )

    def after_core(t):
        core_copy(t).wait_recv()
        nt[t, c] = nt[t, c] + rc[t]
        for k in (2, 1, 3):
            y_copy(t, k).start()

    wsum = jnp.zeros((8, 256), F32)
    full = D // 8
    small_y = []
    tot[...] = jnp.zeros_like(tot)
    for t, j in enumerate(blocks):
        for k in (1, 2, 3):
            x_copy(t, k).wait_recv()
        lanes = pl.ds(pl.multiple_of(j * 128, 128), 128)
        least = jnp.minimum(
            jnp.minimum(lmin[t], rx[0, t]), jnp.minimum(rx[1, t], rx[2, t])
        )
        scale = rtau[:, lanes]
        payoff = jnp.exp(scale * least)
        p = payoff * scale
        tot[pl.ds(j, 1), :] = jnp.sum(payoff, axis=0, keepdims=True)

        def group(g, t=t, p=p):
            ys = [noise[t, g * 8 + s].astype(F32) * p for s in range(8)]
            return sums_of(ys)

        def groups(r, _, group=group):
            for u in range(6):
                g = r * 6 + u
                stage[pl.ds(pl.multiple_of(g * 8, 8), 8), :] = group(g)
            return 0

        lax.fori_loop(0, full // 6, groups, 0)
        for g in range(full // 6 * 6, full):
            stage[g * 8 : g * 8 + 8, :] = group(g)
        rest = [noise[t, full * 8 + s].astype(F32) * p for s in range(D - full * 8)]
        rest += [jnp.zeros((8, 128), F32)] * (8 - len(rest))
        stage[full * 8 : full * 8 + 8, :] = sums_of(rest)
        for h in range(2):
            block = stage[h * 128 : (h + 1) * 128, :].T
            part = jnp.zeros((8, 128), F32)
            for q in range(16):
                zz, yy, cc = q // 8, (q // 2) % 4, q % 2
                piece = block[q * 8 : (q + 1) * 8, :]
                nt[t, cc, yy, zz, :, h * 128 : (h + 1) * 128] = piece
                part = part + piece
            wsum = wsum + (
                jnp.concatenate([part, jnp.zeros((8, 128), F32)], axis=1)
                if h == 0
                else jnp.concatenate([jnp.zeros((8, 128), F32), part], axis=1)
            )
        if t == 0:
            pl.semaphore_wait(know.at[3], 1)
            pl.semaphore_wait(know.at[4], 1)
            tell(know.at[5], z_last)
        if t == 3:
            w = jnp.sum(wsum, axis=0, keepdims=True)
            tot[4:5, :] = w[:, 0:128]
            tot[5:6, :] = w[:, 128:256]
            me = y * NC + c
            smy[me] = tot[...]
            for k in (4, 5, 3, 2, 7, 6, 1):
                cp = pltpu.make_async_remote_copy(
                    src_ref=smy.at[me], dst_ref=smy.at[me], send_sem=smy_s.at[k - 1], recv_sem=smy_r.at[k - 1],
                    device_id=at(z, (y + k // 2) % NY, (c + k) % 2), device_id_type=MESH,
                )
                cp.start()
                small_y.append(cp)
        core_copy(t).start()
        if t >= 1:
            after_core(t - 1)

    pl.semaphore_wait(know.at[5], 1)
    after_core(3)

    def z_copy(t, peer, zz):
        return pltpu.make_async_remote_copy(
            src_ref=nt.at[t, c, y, zz], dst_ref=rz.at[z], send_sem=sz_s.at[peer], recv_sem=sz_r.at[z],
            device_id=at(peer, y, c), device_id_type=MESH,
        )

    def after_y(t):
        for k in range(1, NY):
            y_copy(t, k).wait_recv()
        nt[t, c, y] = nt[t, c, y] + (ry[t, 0] + ry[t, 1] + ry[t, 2])
        base = 2 * ((jz + PAIRS[t]) % 4)
        if PAIRS[t] == 0:
            peer = base + 1 - z % 2
            z_copy(t, peer, 1 - z % 2).start()
        else:
            for zz in range(2):
                z_copy(t, base + zz, zz).start()

    after_y(0)
    for cp in small_y:
        cp.wait_recv()
    smz[z] = ((smy[0] + smy[1]) + (smy[2] + smy[3])) + ((smy[4] + smy[5]) + (smy[6] + smy[7]))
    small_z = []
    for k in (4, 3, 5, 2, 6, 1, 7):
        cp = pltpu.make_async_remote_copy(
            src_ref=smz.at[z], dst_ref=smz.at[z], send_sem=smz_s.at[k - 1], recv_sem=smz_r.at[k - 1],
            device_id=at((z + k) % NZ, y, c), device_id_type=MESH,
        )
        cp.start()
        small_z.append(cp)
    after_y(1)
    after_y(2)
    after_y(3)

    for cp in small_z:
        cp.wait_recv()
    whole = ((smz[0] + smz[1]) + (smz[2] + smz[3])) + ((smz[4] + smz[5]) + (smz[6] + smz[7]))
    inner = K * NZ * NY * NC
    tot[...] = whole
    totals = jnp.concatenate([whole[k : k + 1, :] for k in range(4)], axis=1)
    driver = driver_of(totals * (1.0 / inner))
    rv_ref[...] = jnp.zeros((1, 128), F32) + (
        jnp.sum(totals, axis=1, keepdims=True) * (1.0 / (M * inner))
        + jnp.sum(driver, axis=1, keepdims=True) * (1.0 / M)
    )
    weight = root_t * totals * (1.0 / (M * inner)) + driver / (root_t * M)
    w_hi = weight.astype(BF16).astype(F32)
    w_mid = (weight - w_hi).astype(BF16).astype(F32)
    w_lo = weight - w_hi - w_mid
    rows = lax.broadcasted_iota(jnp.int32, (8, M), 0)
    lhs = jnp.where(rows == 0, w_hi, jnp.where(rows == 1, w_mid, jnp.where(rows == 2, w_lo, 0.0)))
    prod = lax.dot_general(
        lhs.astype(BF16), outer[...], (((1,), (1,)), ((), ())), preferred_element_type=F32
    )
    noise_sum = jnp.sum(prod, axis=0, keepdims=True)
    moment_sum = jnp.concatenate([whole[4:5, :], whole[5:6, :]], axis=1)[:, 0:D]
    rg_ref[...] = (noise_sum + moment_sum * (1.0 / (M * inner))) / (vol_v[...] * start_v[...])
    own_row = tot[pl.ds(path // 16, 1), :] * (1.0 / inner)
    own_row = pltpu.roll(jnp.broadcast_to(own_row, (8, 128)), (128 - (path % 16) * 8) % 128, axis=1)
    pv_ref[...] = own_row[0:1, 0:8]

    own = nt[3, c, y, z % 2]
    for k in range(1, NZ):
        src = (z + k) % NZ
        pltpu.make_async_remote_copy(
            src_ref=rz.at[src], dst_ref=rz.at[src], send_sem=sz_s.at[src], recv_sem=sz_r.at[src],
            device_id=at(src, y, c), device_id_type=MESH,
        ).wait_recv()
        own = own + rz[src]
    pg_ref[...] = own[:, 0:D] * dinv[...]

    for cp in small_y + small_z:
        cp.wait_send()
    for t in range(4):
        core_copy(t).wait_send()
        for k in (1, 2, 3):
            x_copy(t, k).wait_send()
        for k in range(1, NY):
            y_copy(t, k).wait_send()
    for k in range(1, NZ):
        peer = (z + k) % NZ
        pltpu.make_async_remote_copy(
            src_ref=rz.at[peer], dst_ref=rz.at[peer], send_sem=sz_s.at[peer], recv_sem=sz_r.at[peer],
            device_id=at(peer, y, c), device_id_type=MESH,
        ).wait_send()


def hand_out(a, b, c, d, a_out, b_out, c_out, d_out, one, sem):
    one[...] = a[0:1, 0:1]
    pairs = ((d, d_out), (b, b_out), (c, c_out), (one, a_out))
    copies = [pltpu.make_async_copy(src, dst, sem.at[k]) for k, (src, dst) in enumerate(pairs)]
    for cp in copies:
        cp.start()
    for cp in copies:
        cp.wait()


def per_device(inner_noise, outer_noise, start, vol, times):
    K, D, M = inner_noise.shape
    hbm = pl.BlockSpec(memory_space=pltpu.HBM)
    vmem = pl.BlockSpec(memory_space=pltpu.VMEM)
    dma = pltpu.SemaphoreType.DMA
    V = pltpu.VMEM
    results = pl.pallas_call(
        kernel,
        out_shape=(V((1, 128), F32), V((1, D), F32), V((1, 8), F32), V((8, D), F32)),
        in_specs=[hbm] * 5,
        out_specs=(vmem,) * 4,
        scratch_shapes=[
            V((4, D, K, 128), BF16), V((D, M), BF16), V((1, D), F32), V((1, D), F32), V((1, M), F32),
            V((1, 256), F32), V((1, 256), F32), V((256, 128), F32), V((4, 256, 128), F32),
            V((4, K, 128), F32), V((3, 4, K, 128), F32), V((1, M), F32), V((256, 128), F32),
            V((4, NC, NY, 2, 8, 256), F32), V((4, NY, 2, 8, 256), F32),
            V((4, 3, 2, 8, 256), F32), V((NZ, 8, 256), F32),
            V((NY * NC, 8, 128), F32), V((NZ, 8, 128), F32), V((8, 128), F32),
            V((8, D), F32),
            dma((8,)), dma((12,)), dma((12,)), dma((4,)), dma((4,)), dma((12,)), dma((12,)),
            dma((NZ,)), dma((NZ,)), dma((7,)), dma((7,)), dma((7,)), dma((7,)),
            pltpu.SemaphoreType.REGULAR((6,)),
        ],
        compiler_params=pltpu.CompilerParams(
            collective_id=0, has_side_effects=True
        ),
    )(
        jnp.transpose(inner_noise, (1, 0, 2)), outer_noise, start[None], vol[None], times[None]
    )
    root_value, root_grad, point_value, point_grad = pl.pallas_call(
        hand_out,
        out_shape=tuple(jax.ShapeDtypeStruct(s, F32) for s in ((1, 1), (1, D), (1, 8), (8, D))),
        in_specs=[vmem] * 4,
        out_specs=(hbm,) * 4,
        scratch_shapes=[V((1, 1), F32), dma((4,))],
        compiler_params=pltpu.CompilerParams(vmem_limit_bytes=1024 * 1024),
    )(*results)
    return root_value[0], root_grad[0], point_value[0], point_grad.T


def solution(mesh):
    in_specs = (P("path", "dim", None), P("dim", None), P("dim"), P("dim"), P())
    out_specs = (P(), P("dim"), P("path"), P("dim", "path"))
    return jax.shard_map(
        per_device, mesh=mesh, in_specs=in_specs, out_specs=out_specs, check_vma=False
    )
```

```python
import functools

import jax
import jax.numpy as jnp
from jax import lax
from jax.experimental import pallas as pl
from jax.experimental.pallas import tpu as pltpu
from jax.sharding import PartitionSpec as P

drift = 0.02
delta = 2.0 / 3.0
rate_free = 0.02
gamma_high = 0.2
gamma_low = 0.02
value_high = 0.4
value_low = 0.7

NX, NY, NZ, NC = 4, 4, 8, 2
MESH = pl.DeviceIdType.MESH
F32 = jnp.float32
BF16 = jnp.bfloat16
PAIRS = (2, 1, 3, 0)


def driver_of(value):
    slope = jnp.clip((value - value_high) / (value_low - value_high), 0.0, 1.0)
    quota = gamma_high + (gamma_low - gamma_high) * slope
    return -(1.0 - delta) * quota * value - rate_free * value


def smallest(terms):
    while len(terms) > 1:
        pairs = [jnp.minimum(a, b) for a, b in zip(terms[::2], terms[1::2])]
        terms = pairs + terms[len(pairs) * 2 :]
    return terms[0]


def kernel(
    noise_hbm, outer_hbm, start_hbm, vol_hbm, times_hbm,
    rv_ref, rg_ref, pv_ref, pg_ref,
    noise, outer, start_v, vol_v, times_v,
    startp, volp, volb, abase, lmin, rx, rtau, stage, nt, rc, ry, rz, smy, smz, tot, dinv,
    in_sem, sx_s, sx_r, sc_s, sc_r, sy_s, sy_r, sz_s, sz_r, smy_s, smy_r, smz_s, smz_r, know,
):
    D, K, M = noise_hbm.shape
    path = lax.axis_index("path")
    x = lax.axis_index("dim")
    z = path // (NY * NC)
    y = (path // NC) % NY
    c = path % NC
    jz = z // 2

    def at_x(k):
        return (path, (x + k) % NX)

    def at(zz, yy, cc):
        return ((zz * NY + yy) * NC + cc, x)

    small_in = [
        pltpu.make_async_copy(vol_hbm, vol_v, in_sem.at[0]),
        pltpu.make_async_copy(start_hbm, start_v, in_sem.at[1]),
        pltpu.make_async_copy(times_hbm, times_v, in_sem.at[2]),
        pltpu.make_async_copy(outer_hbm, outer, in_sem.at[3]),
    ]
    for cp in small_in:
        cp.start()
    blocks = [(jz + off) % 4 for off in PAIRS]
    noise_in = [
        pltpu.make_async_copy(
            noise_hbm.at[:, :, pl.ds(pl.multiple_of(j * 128, 128), 128)], noise.at[t], in_sem.at[4 + t]
        )
        for t, j in enumerate(blocks)
    ]
    for cp in noise_in:
        cp.start()
    barrier = pltpu.get_barrier_semaphore()
    near = [at((z + k) % NZ, y, c) for k in (1, NZ - 1)]
    near += [at(z, (y + k) % NY, cc) for k in (1, NY - 1) for cc in (c, 1 - c)]
    near += [at_x(k) for k in (1, 2, 3)] + [at(z, y, 1 - c)]
    for peer in near:
        pl.semaphore_signal(barrier, inc=1, device_id=peer, device_id_type=MESH)

    def tell(sem, peer):
        pl.semaphore_signal(sem, inc=1, device_id=peer, device_id_type=MESH)

    z_next, z_last = at((z + 1) % NZ, y, c), at((z + NZ - 1) % NZ, y, c)

    for cp in small_in:
        cp.wait()

    startp[...] = jnp.ones_like(startp)
    volp[...] = jnp.ones_like(volp)
    startp[:, 0:D] = start_v[...]
    volp[:, 0:D] = vol_v[...]
    vol = volp[...]
    begin = startp[...]
    times = times_v[...]
    tau = 1.0 - times
    root_t = jnp.sqrt(times)
    root_tau = jnp.sqrt(tau)
    inv_root_tau = 1.0 / root_tau
    offset = jnp.log(begin) + (drift - 0.5 * vol * vol)
    for h in range(2):
        volb[h * 128 : (h + 1) * 128, :] = jnp.broadcast_to(
            vol[:, h * 128 : (h + 1) * 128], (128, 128)
        ).T
        stage[h * 128 : (h + 1) * 128, :] = jnp.broadcast_to(
            offset[:, h * 128 : (h + 1) * 128], (128, 128)
        ).T
    for lo in range(0, D, 16):
        hi = min(lo + 16, D)
        for j in range(4):
            ls = slice(j * 128, (j + 1) * 128)
            o = outer[lo:hi, ls].astype(F32)
            abase[j, lo:hi, :] = (
                stage[lo:hi, :] + volb[lo:hi, :] * (root_t[:, ls] * o)
            ) * inv_root_tau[:, ls]

    def x_copy(t, k):
        return pltpu.make_async_remote_copy(
            src_ref=lmin.at[t], dst_ref=rx.at[k - 1, t],
            send_sem=sx_s.at[t * 3 + k - 1], recv_sem=sx_r.at[t * 3 + k - 1],
            device_id=at_x(k), device_id_type=MESH,
        )

    unroll = 25
    for t in (0, 2):
        noise_in[t].wait()
        noise_in[t + 1].wait()

        def body(g, acc, t=t):
            terms = [[], []]
            for u in range(unroll):
                d = g * unroll + u
                v = volb[pl.ds(d, K, stride=0), :]
                for h in range(2):
                    n = noise[t + h, d].astype(F32)
                    terms[h].append(n * v + abase[blocks[t + h], pl.ds(d, K, stride=0), :])
            return tuple(jnp.minimum(a, smallest(r)) for a, r in zip(acc, terms))

        acc = lax.fori_loop(0, D // unroll, body, (jnp.full((K, 128), 3.0e38, F32),) * 2)
        lmin[t], lmin[t + 1] = acc
        if t == 0:
            pl.semaphore_wait(barrier, len(near))
            tell(know.at[0], at(z, (y + NY - 1) % NY, c))
            tell(know.at[1], z_last)
            tell(know.at[2], z_next)
        for h in range(2):
            for k in (2, 1, 3):
                x_copy(t + h, k).start()

    lane = lax.broadcasted_iota(jnp.int32, (K, M), 1)
    row = lax.broadcasted_iota(jnp.int32, (K, M), 0)
    pick = lane == path * K + row
    own_t = jnp.sum(jnp.where(pick, times, 0.0), axis=1, keepdims=True)
    own_outer = lax.dot_general(
        jnp.where(pick, 1.0, 0.0).astype(BF16), outer[...], (((1,), (1,)), ((), ())),
        preferred_element_type=F32,
    )
    vol_d = vol_v[...]
    own_state = start_v[...] * jnp.exp(
        (drift - 0.5 * vol_d * vol_d) * own_t + vol_d * jnp.sqrt(own_t) * own_outer
    )
    dinv[...] = 1.0 / ((K * NZ * NY * NC) * vol_d * own_state * (1.0 - own_t))

    rtau[...] = root_tau

    sub = lax.broadcasted_iota(jnp.int32, (8, 128), 0)
    bit2 = (sub & 4) == 0
    bit1 = (sub & 2) == 0
    bit0 = (sub & 1) == 0

    def merge(a, b, first, shift):
        if shift == 4:
            return jnp.where(first, a, b) + pltpu.roll(jnp.where(first, b, a), 4, axis=0)
        return jnp.where(
            first,
            a + pltpu.roll(a, 8 - shift, axis=0),
            b + pltpu.roll(b, shift, axis=0),
        )

    def sums_of(ys):
        c4 = [merge(ys[s], ys[s + 4], bit2, 4) for s in range(4)]
        e2 = [merge(c4[s], c4[s + 2], bit1, 2) for s in range(2)]
        return merge(e2[0], e2[1], bit0, 1)

    pl.semaphore_wait(know.at[0], 1)
    pl.semaphore_wait(know.at[1], 1)
    pl.semaphore_wait(know.at[2], 1)
    tell(know.at[3], z_last)
    tell(know.at[4], z_next)

    def core_copy(t):
        return pltpu.make_async_remote_copy(
            src_ref=nt.at[t, 1 - c], dst_ref=rc.at[t], send_sem=sc_s.at[t], recv_sem=sc_r.at[t],
            device_id=at(z, y, 1 - c), device_id_type=MESH,
        )

    def y_copy(t, k):
        peer = (y + k) % NY
        return pltpu.make_async_remote_copy(
            src_ref=nt.at[t, c, peer], dst_ref=ry.at[t, k - 1],
            send_sem=sy_s.at[t * 3 + k - 1], recv_sem=sy_r.at[t * 3 + k - 1],
            device_id=at(z, peer, c), device_id_type=MESH,
        )

    def after_core(t):
        core_copy(t).wait_recv()
        nt[t, c] = nt[t, c] + rc[t]
        for k in (2, 1, 3):
            y_copy(t, k).start()

    wsum = jnp.zeros((8, 256), F32)
    full = D // 8
    small_y = []
    tot[...] = jnp.zeros_like(tot)
    for t, j in enumerate(blocks):
        for k in (1, 2, 3):
            x_copy(t, k).wait_recv()
        lanes = pl.ds(pl.multiple_of(j * 128, 128), 128)
        least = jnp.minimum(
            jnp.minimum(lmin[t], rx[0, t]), jnp.minimum(rx[1, t], rx[2, t])
        )
        scale = rtau[:, lanes]
        payoff = jnp.exp(scale * least)
        p = payoff * scale
        tot[pl.ds(j, 1), :] = jnp.sum(payoff, axis=0, keepdims=True)

        def group(g, t=t, p=p):
            ys = [noise[t, g * 8 + s].astype(F32) * p for s in range(8)]
            return sums_of(ys)

        def groups(r, _, group=group):
            for u in range(6):
                g = r * 6 + u
                stage[pl.ds(pl.multiple_of(g * 8, 8), 8), :] = group(g)
            return 0

        lax.fori_loop(0, full // 6, groups, 0)
        for g in range(full // 6 * 6, full):
            stage[g * 8 : g * 8 + 8, :] = group(g)
        rest = [noise[t, full * 8 + s].astype(F32) * p for s in range(D - full * 8)]
        rest += [jnp.zeros((8, 128), F32)] * (8 - len(rest))
        stage[full * 8 : full * 8 + 8, :] = sums_of(rest)
        for h in range(2):
            block = stage[h * 128 : (h + 1) * 128, :].T
            part = jnp.zeros((8, 128), F32)
            for q in range(16):
                zz, yy, cc = q // 8, (q // 2) % 4, q % 2
                piece = block[q * 8 : (q + 1) * 8, :]
                nt[t, cc, yy, zz, :, h * 128 : (h + 1) * 128] = piece
                part = part + piece
            wsum = wsum + (
                jnp.concatenate([part, jnp.zeros((8, 128), F32)], axis=1)
                if h == 0
                else jnp.concatenate([jnp.zeros((8, 128), F32), part], axis=1)
            )
        if t == 0:
            pl.semaphore_wait(know.at[3], 1)
            pl.semaphore_wait(know.at[4], 1)
            tell(know.at[5], z_last)
        if t == 3:
            w = jnp.sum(wsum, axis=0, keepdims=True)
            tot[4:5, :] = w[:, 0:128]
            tot[5:6, :] = w[:, 128:256]
            me = y * NC + c
            smy[me] = tot[...]
            for k in (4, 5, 3, 2, 7, 6, 1):
                cp = pltpu.make_async_remote_copy(
                    src_ref=smy.at[me], dst_ref=smy.at[me], send_sem=smy_s.at[k - 1], recv_sem=smy_r.at[k - 1],
                    device_id=at(z, (y + k // 2) % NY, (c + k) % 2), device_id_type=MESH,
                )
                cp.start()
                small_y.append(cp)
        core_copy(t).start()

    for t in range(3):
        after_core(t)
    after_core(3)

    def z_copy(t, peer, zz):
        return pltpu.make_async_remote_copy(
            src_ref=nt.at[t, c, y, zz], dst_ref=rz.at[z], send_sem=sz_s.at[peer], recv_sem=sz_r.at[z],
            device_id=at(peer, y, c), device_id_type=MESH,
        )

    def after_y(t):
        for k in range(1, NY):
            y_copy(t, k).wait_recv()
        nt[t, c, y] = nt[t, c, y] + (ry[t, 0] + ry[t, 1] + ry[t, 2])
        base = 2 * ((jz + PAIRS[t]) % 4)
        if PAIRS[t] == 0:
            peer = base + 1 - z % 2
            z_copy(t, peer, 1 - z % 2).start()
        else:
            for zz in range(2):
                z_copy(t, base + zz, zz).start()

    pl.semaphore_wait(know.at[5], 1)
    for cp in small_y:
        cp.wait_recv()
    smz[z] = ((smy[0] + smy[1]) + (smy[2] + smy[3])) + ((smy[4] + smy[5]) + (smy[6] + smy[7]))
    small_z = []
    for k in (4, 3, 5, 2, 6, 1, 7):
        cp = pltpu.make_async_remote_copy(
            src_ref=smz.at[z], dst_ref=smz.at[z], send_sem=smz_s.at[k - 1], recv_sem=smz_r.at[k - 1],
            device_id=at((z + k) % NZ, y, c), device_id_type=MESH,
        )
        cp.start()
        small_z.append(cp)
    after_y(0)
    after_y(1)
    after_y(2)
    after_y(3)

    for cp in small_z:
        cp.wait_recv()
    whole = ((smz[0] + smz[1]) + (smz[2] + smz[3])) + ((smz[4] + smz[5]) + (smz[6] + smz[7]))
    inner = K * NZ * NY * NC
    tot[...] = whole
    totals = jnp.concatenate([whole[k : k + 1, :] for k in range(4)], axis=1)
    driver = driver_of(totals * (1.0 / inner))
    rv_ref[...] = jnp.zeros((1, 128), F32) + (
        jnp.sum(totals, axis=1, keepdims=True) * (1.0 / (M * inner))
        + jnp.sum(driver, axis=1, keepdims=True) * (1.0 / M)
    )
    weight = root_t * totals * (1.0 / (M * inner)) + driver / (root_t * M)
    w_hi = weight.astype(BF16).astype(F32)
    w_mid = (weight - w_hi).astype(BF16).astype(F32)
    w_lo = weight - w_hi - w_mid
    rows = lax.broadcasted_iota(jnp.int32, (8, M), 0)
    lhs = jnp.where(rows == 0, w_hi, jnp.where(rows == 1, w_mid, jnp.where(rows == 2, w_lo, 0.0)))
    prod = lax.dot_general(
        lhs.astype(BF16), outer[...], (((1,), (1,)), ((), ())), preferred_element_type=F32
    )
    noise_sum = jnp.sum(prod, axis=0, keepdims=True)
    moment_sum = jnp.concatenate([whole[4:5, :], whole[5:6, :]], axis=1)[:, 0:D]
    rg_ref[...] = (noise_sum + moment_sum * (1.0 / (M * inner))) / (vol_v[...] * start_v[...])
    own_row = tot[pl.ds(path // 16, 1), :] * (1.0 / inner)
    own_row = pltpu.roll(jnp.broadcast_to(own_row, (8, 128)), (128 - (path % 16) * 8) % 128, axis=1)
    pv_ref[...] = own_row[0:1, 0:8]

    own = nt[3, c, y, z % 2]
    for k in range(1, NZ):
        src = (z + k) % NZ
        pltpu.make_async_remote_copy(
            src_ref=rz.at[src], dst_ref=rz.at[src], send_sem=sz_s.at[src], recv_sem=sz_r.at[src],
            device_id=at(src, y, c), device_id_type=MESH,
        ).wait_recv()
        own = own + rz[src]
    pg_ref[...] = own[:, 0:D] * dinv[...]

    for cp in small_y + small_z:
        cp.wait_send()
    for t in range(4):
        core_copy(t).wait_send()
        for k in (1, 2, 3):
            x_copy(t, k).wait_send()
        for k in range(1, NY):
            y_copy(t, k).wait_send()
    for k in range(1, NZ):
        peer = (z + k) % NZ
        pltpu.make_async_remote_copy(
            src_ref=rz.at[peer], dst_ref=rz.at[peer], send_sem=sz_s.at[peer], recv_sem=sz_r.at[peer],
            device_id=at(peer, y, c), device_id_type=MESH,
        ).wait_send()


def hand_out(a, b, c, d, a_out, b_out, c_out, d_out, one, sem):
    one[...] = a[0:1, 0:1]
    pairs = ((d, d_out), (b, b_out), (c, c_out), (one, a_out))
    copies = [pltpu.make_async_copy(src, dst, sem.at[k]) for k, (src, dst) in enumerate(pairs)]
    for cp in copies:
        cp.start()
    for cp in copies:
        cp.wait()


def per_device(inner_noise, outer_noise, start, vol, times):
    K, D, M = inner_noise.shape
    hbm = pl.BlockSpec(memory_space=pltpu.HBM)
    vmem = pl.BlockSpec(memory_space=pltpu.VMEM)
    dma = pltpu.SemaphoreType.DMA
    V = pltpu.VMEM
    results = pl.pallas_call(
        kernel,
        out_shape=(V((1, 128), F32), V((1, D), F32), V((1, 8), F32), V((8, D), F32)),
        in_specs=[hbm] * 5,
        out_specs=(vmem,) * 4,
        scratch_shapes=[
            V((4, D, K, 128), BF16), V((D, M), BF16), V((1, D), F32), V((1, D), F32), V((1, M), F32),
            V((1, 256), F32), V((1, 256), F32), V((256, 128), F32), V((4, 256, 128), F32),
            V((4, K, 128), F32), V((3, 4, K, 128), F32), V((1, M), F32), V((256, 128), F32),
            V((4, NC, NY, 2, 8, 256), F32), V((4, NY, 2, 8, 256), F32),
            V((4, 3, 2, 8, 256), F32), V((NZ, 8, 256), F32),
            V((NY * NC, 8, 128), F32), V((NZ, 8, 128), F32), V((8, 128), F32),
            V((8, D), F32),
            dma((8,)), dma((12,)), dma((12,)), dma((4,)), dma((4,)), dma((12,)), dma((12,)),
            dma((NZ,)), dma((NZ,)), dma((7,)), dma((7,)), dma((7,)), dma((7,)),
            pltpu.SemaphoreType.REGULAR((6,)),
        ],
        compiler_params=pltpu.CompilerParams(
            collective_id=0, has_side_effects=True
        ),
    )(
        jnp.transpose(inner_noise, (1, 0, 2)), outer_noise, start[None], vol[None], times[None]
    )
    root_value, root_grad, point_value, point_grad = pl.pallas_call(
        hand_out,
        out_shape=tuple(jax.ShapeDtypeStruct(s, F32) for s in ((1, 1), (1, D), (1, 8), (8, D))),
        in_specs=[vmem] * 4,
        out_specs=(hbm,) * 4,
        scratch_shapes=[V((1, 1), F32), dma((4,))],
        compiler_params=pltpu.CompilerParams(vmem_limit_bytes=1024 * 1024),
    )(*results)
    return root_value[0], root_grad[0], point_value[0], point_grad.T


def solution(mesh):
    in_specs = (P("path", "dim", None), P("dim", None), P("dim"), P("dim"), P())
    out_specs = (P(), P("dim"), P("path"), P("dim", "path"))
    return jax.shard_map(
        per_device, mesh=mesh, in_specs=in_specs, out_specs=out_specs, check_vma=False
    )
```

```python
import functools

import jax
import jax.numpy as jnp
from jax import lax
from jax.experimental import pallas as pl
from jax.experimental.pallas import tpu as pltpu
from jax.sharding import PartitionSpec as P

drift = 0.02
delta = 2.0 / 3.0
rate_free = 0.02
gamma_high = 0.2
gamma_low = 0.02
value_high = 0.4
value_low = 0.7

NX, NY, NZ, NC = 4, 4, 8, 2
MESH = pl.DeviceIdType.MESH
F32 = jnp.float32
BF16 = jnp.bfloat16
CHUNKS = 5


def driver_of(value):
    slope = jnp.clip((value - value_high) / (value_low - value_high), 0.0, 1.0)
    quota = gamma_high + (gamma_low - gamma_high) * slope
    return -(1.0 - delta) * quota * value - rate_free * value


def smallest(terms):
    while len(terms) > 1:
        pairs = [jnp.minimum(a, b) for a, b in zip(terms[::2], terms[1::2])]
        terms = pairs + terms[len(pairs) * 2 :]
    return terms[0]


def kernel(
    noise_hbm, outer_hbm, start_hbm, vol_hbm, times_hbm,
    rv_ref, rg_ref, pv_ref, pg_ref,
    noise, outer, start_v, vol_v, times_v,
    startp, volp, volb, abase, lmin, rx, rows_t, stage, nt, rc, ry, rz, smy, smz, tot, dinv,
    in_sem, sx_s, sx_r, sc_s, sc_r, sy_s, sy_r, sz_s, sz_r, smy_s, smy_r, smz_s, smz_r, know,
):
    D, K, M = noise_hbm.shape
    path = lax.axis_index("path")
    x = lax.axis_index("dim")
    z = path // (NY * NC)
    y = (path // NC) % NY
    c = path % NC
    jz = z // 2

    def at_x(k):
        return (path, (x + k) % NX)

    def at(zz, yy, cc):
        return ((zz * NY + yy) * NC + cc, x)

    small_in = [
        pltpu.make_async_copy(vol_hbm, vol_v, in_sem.at[0]),
        pltpu.make_async_copy(start_hbm, start_v, in_sem.at[1]),
        pltpu.make_async_copy(times_hbm, times_v, in_sem.at[2]),
    ]
    for cp in small_in:
        cp.start()
    odd = z % 2
    blocks = [(jz + off) % 4 for off in (2, 1 + 2 * odd, 3 - 2 * odd, 0)]

    def lanes_of(t):
        return pl.ds(pl.multiple_of(blocks[t] * 128, 128), 128)

    per = D // CHUNKS
    outer_in = [
        pltpu.make_async_copy(outer_hbm.at[:, lanes_of(t)], outer.at[:, lanes_of(t)], in_sem.at[3 + t])
        for t in range(4)
    ]
    noise_in = [
        [
            pltpu.make_async_copy(
                noise_hbm.at[pl.ds(q * per, per), :, lanes_of(t)],
                noise.at[t, pl.ds(q * per, per)],
                in_sem.at[7 + t * CHUNKS + q],
            )
            for q in range(CHUNKS)
        ]
        for t in range(4)
    ]
    for cp in [outer_in[0]] + noise_in[0]:
        cp.start()

    barrier = pltpu.get_barrier_semaphore()
    near = [at((z + k) % NZ, y, c) for k in (1, NZ - 1)]
    near += [at(z, (y + k) % NY, cc) for k in (1, NY - 1) for cc in (c, 1 - c)]
    near += [at_x(k) for k in (1, 2, 3)] + [at(z, y, 1 - c)]
    for peer in near:
        pl.semaphore_signal(barrier, inc=1, device_id=peer, device_id_type=MESH)

    def tell(sem, peer):
        pl.semaphore_signal(sem, inc=1, device_id=peer, device_id_type=MESH)

    z_next, z_last = at((z + 1) % NZ, y, c), at((z + NZ - 1) % NZ, y, c)

    for t in range(1, 4):
        for cp in [outer_in[t]] + noise_in[t]:
            cp.start()
    for cp in small_in:
        cp.wait()

    startp[...] = jnp.ones_like(startp)
    volp[...] = jnp.ones_like(volp)
    startp[:, 0:D] = start_v[...]
    volp[:, 0:D] = vol_v[...]
    vol = volp[...]
    begin = startp[...]
    times = times_v[...]
    tau = 1.0 - times
    root_t = jnp.sqrt(times)
    root_tau = jnp.sqrt(tau)
    inv_root_tau = 1.0 / root_tau
    offset = jnp.log(begin) + (drift - 0.5 * vol * vol)
    for h in range(2):
        volb[h * 128 : (h + 1) * 128, :] = jnp.broadcast_to(
            vol[:, h * 128 : (h + 1) * 128], (128, 128)
        ).T
        stage[h * 128 : (h + 1) * 128, :] = jnp.broadcast_to(
            offset[:, h * 128 : (h + 1) * 128], (128, 128)
        ).T
    rows_t[0:1, :] = root_t
    rows_t[1:2, :] = root_tau
    rows_t[2:3, :] = inv_root_tau

    def coefficients(t):
        outer_in[t].wait()
        scale = rows_t[0:1, lanes_of(t)]
        inv = rows_t[2:3, lanes_of(t)]
        for lo in range(0, D, 16):
            hi = min(lo + 16, D)
            o = outer[lo:hi, lanes_of(t)].astype(F32)
            abase[t, lo:hi, :] = (stage[lo:hi, :] + volb[lo:hi, :] * (scale * o)) * inv

    def x_copy(t, k):
        return pltpu.make_async_remote_copy(
            src_ref=lmin.at[t], dst_ref=rx.at[k - 1, t],
            send_sem=sx_s.at[t * 3 + k - 1], recv_sem=sx_r.at[t * 3 + k - 1],
            device_id=at_x(k), device_id_type=MESH,
        )

    def minimum_of(ts):
        acc = [jnp.full((K, 128), 3.0e38, F32) for _ in ts]
        for q in range(CHUNKS):
            terms = [[] for _ in ts]
            for t in ts:
                noise_in[t][q].wait()
            for d in range(q * per, (q + 1) * per):
                v = volb[pl.ds(d, K, stride=0), :]
                for row, t in zip(terms, ts):
                    row.append(noise[t, d].astype(F32) * v + abase[t, pl.ds(d, K, stride=0), :])
            acc = [jnp.minimum(a, smallest(r)) for a, r in zip(acc, terms)]
        for t, a in zip(ts, acc):
            lmin[t] = a

    for ts in ((0,), (1,), (2, 3)):
        for t in ts:
            coefficients(t)
        minimum_of(ts)
        if ts[0] == 0:
            pl.semaphore_wait(barrier, len(near))
            tell(know.at[0], at(z, (y + NY - 1) % NY, c))
            tell(know.at[1], z_last)
            tell(know.at[2], z_next)
        for t in ts:
            for k in (2, 1, 3):
                x_copy(t, k).start()

    lane = lax.broadcasted_iota(jnp.int32, (K, M), 1)
    row = lax.broadcasted_iota(jnp.int32, (K, M), 0)
    pick = lane == path * K + row
    own_t = jnp.sum(jnp.where(pick, times, 0.0), axis=1, keepdims=True)
    own_outer = lax.dot_general(
        jnp.where(pick, 1.0, 0.0).astype(BF16), outer[...], (((1,), (1,)), ((), ())),
        preferred_element_type=F32,
    )
    vol_d = vol_v[...]
    own_state = start_v[...] * jnp.exp(
        (drift - 0.5 * vol_d * vol_d) * own_t + vol_d * jnp.sqrt(own_t) * own_outer
    )
    dinv[...] = 1.0 / ((K * NZ * NY * NC) * vol_d * own_state * (1.0 - own_t))

    sub = lax.broadcasted_iota(jnp.int32, (8, 128), 0)
    bit2 = (sub & 4) == 0
    bit1 = (sub & 2) == 0
    bit0 = (sub & 1) == 0

    def merge(a, b, first, shift):
        if shift == 4:
            return jnp.where(first, a, b) + pltpu.roll(jnp.where(first, b, a), 4, axis=0)
        return jnp.where(
            first,
            a + pltpu.roll(a, 8 - shift, axis=0),
            b + pltpu.roll(b, shift, axis=0),
        )

    def sums_of(ys):
        c4 = [merge(ys[s], ys[s + 4], bit2, 4) for s in range(4)]
        e2 = [merge(c4[s], c4[s + 2], bit1, 2) for s in range(2)]
        return merge(e2[0], e2[1], bit0, 1)

    pl.semaphore_wait(know.at[0], 1)
    pl.semaphore_wait(know.at[1], 1)
    pl.semaphore_wait(know.at[2], 1)
    tell(know.at[3], z_last)
    tell(know.at[4], z_next)

    def core_copy(t):
        return pltpu.make_async_remote_copy(
            src_ref=nt.at[t, 1 - c], dst_ref=rc.at[t], send_sem=sc_s.at[t], recv_sem=sc_r.at[t],
            device_id=at(z, y, 1 - c), device_id_type=MESH,
        )

    def y_copy(t, k):
        peer = (y + k) % NY
        return pltpu.make_async_remote_copy(
            src_ref=nt.at[t, c, peer], dst_ref=ry.at[t, k - 1],
            send_sem=sy_s.at[t * 3 + k - 1], recv_sem=sy_r.at[t * 3 + k - 1],
            device_id=at(z, peer, c), device_id_type=MESH,
        )

    def after_core(t):
        core_copy(t).wait_recv()
        nt[t, c] = nt[t, c] + rc[t]
        for k in (2, 1, 3):
            y_copy(t, k).start()

    wsum = [jnp.zeros((8, 128), F32)] * 2
    small_y = []
    tot[...] = jnp.zeros_like(tot)
    for t, j in enumerate(blocks):
        for k in (1, 2, 3):
            x_copy(t, k).wait_recv()
        least = jnp.minimum(
            jnp.minimum(lmin[t], rx[0, t]), jnp.minimum(rx[1, t], rx[2, t])
        )
        scale = rows_t[1:2, lanes_of(t)]
        payoff = jnp.exp(scale * least)
        p = payoff * scale
        tot[pl.ds(j, 1), :] = jnp.sum(payoff, axis=0, keepdims=True)
        for h in range(2):
            tiles = []
            for g in range(16):
                first = h * 128 + g * 8
                ys = [noise[t, first + s].astype(F32) * p for s in range(min(8, D - first))]
                ys += [jnp.zeros((8, 128), F32)] * (8 - len(ys))
                tiles.append(sums_of(ys))
            block = jnp.concatenate(tiles, axis=0).T
            part = jnp.zeros((8, 128), F32)
            for q in range(16):
                zz, yy, cc = q // 8, (q // 2) % 4, q % 2
                piece = block[q * 8 : (q + 1) * 8, :]
                nt[t, cc, yy, zz, :, h * 128 : (h + 1) * 128] = piece
                part = part + piece
            wsum[h] = wsum[h] + part
        if t == 0:
            pl.semaphore_wait(know.at[3], 1)
            pl.semaphore_wait(know.at[4], 1)
            tell(know.at[5], z_last)
        if t == 3:
            for h in range(2):
                tot[4 + h : 5 + h, :] = jnp.sum(wsum[h], axis=0, keepdims=True)
            me = y * NC + c
            smy[me] = tot[...]
            for k in (4, 5, 3, 2, 7, 6, 1):
                cp = pltpu.make_async_remote_copy(
                    src_ref=smy.at[me], dst_ref=smy.at[me], send_sem=smy_s.at[k - 1], recv_sem=smy_r.at[k - 1],
                    device_id=at(z, (y + k // 2) % NY, (c + k) % 2), device_id_type=MESH,
                )
                cp.start()
                small_y.append(cp)
        core_copy(t).start()

    for t in range(3):
        after_core(t)
    after_core(3)

    def z_copy(t, peer, zz):
        return pltpu.make_async_remote_copy(
            src_ref=nt.at[t, c, y, zz], dst_ref=rz.at[z], send_sem=sz_s.at[peer], recv_sem=sz_r.at[z],
            device_id=at(peer, y, c), device_id_type=MESH,
        )

    def after_y(t):
        for k in range(1, NY):
            y_copy(t, k).wait_recv()
        nt[t, c, y] = nt[t, c, y] + (ry[t, 0] + ry[t, 1] + ry[t, 2])
        base = 2 * blocks[t]
        if t == 3:
            z_copy(t, base + 1 - odd, 1 - odd).start()
        else:
            for zz in range(2):
                z_copy(t, base + zz, zz).start()

    pl.semaphore_wait(know.at[5], 1)
    for cp in small_y:
        cp.wait_recv()
    smz[z] = ((smy[0] + smy[1]) + (smy[2] + smy[3])) + ((smy[4] + smy[5]) + (smy[6] + smy[7]))
    small_z = []
    for k in (4, 3, 5, 2, 6, 1, 7):
        cp = pltpu.make_async_remote_copy(
            src_ref=smz.at[z], dst_ref=smz.at[z], send_sem=smz_s.at[k - 1], recv_sem=smz_r.at[k - 1],
            device_id=at((z + k) % NZ, y, c), device_id_type=MESH,
        )
        cp.start()
        small_z.append(cp)
    after_y(0)
    after_y(1)
    after_y(2)
    after_y(3)

    for cp in small_z:
        cp.wait_recv()
    whole = ((smz[0] + smz[1]) + (smz[2] + smz[3])) + ((smz[4] + smz[5]) + (smz[6] + smz[7]))
    inner = K * NZ * NY * NC
    tot[...] = whole
    totals = jnp.concatenate([whole[k : k + 1, :] for k in range(4)], axis=1)
    driver = driver_of(totals * (1.0 / inner))
    rv_ref[...] = jnp.zeros((1, 128), F32) + (
        jnp.sum(totals, axis=1, keepdims=True) * (1.0 / (M * inner))
        + jnp.sum(driver, axis=1, keepdims=True) * (1.0 / M)
    )
    weight = root_t * totals * (1.0 / (M * inner)) + driver / (root_t * M)
    w_hi = weight.astype(BF16).astype(F32)
    w_mid = (weight - w_hi).astype(BF16).astype(F32)
    w_lo = weight - w_hi - w_mid
    rows = lax.broadcasted_iota(jnp.int32, (8, M), 0)
    lhs = jnp.where(rows == 0, w_hi, jnp.where(rows == 1, w_mid, jnp.where(rows == 2, w_lo, 0.0)))
    prod = lax.dot_general(
        lhs.astype(BF16), outer[...], (((1,), (1,)), ((), ())), preferred_element_type=F32
    )
    noise_sum = jnp.sum(prod, axis=0, keepdims=True)
    moment_sum = jnp.concatenate([whole[4:5, :], whole[5:6, :]], axis=1)[:, 0:D]
    rg_ref[...] = (noise_sum + moment_sum * (1.0 / (M * inner))) / (vol_v[...] * start_v[...])
    own_row = tot[pl.ds(path // 16, 1), :] * (1.0 / inner)
    own_row = pltpu.roll(jnp.broadcast_to(own_row, (8, 128)), (128 - (path % 16) * 8) % 128, axis=1)
    pv_ref[...] = own_row[0:1, 0:8]

    own = nt[3, c, y, odd]
    for k in range(1, NZ):
        src = (z + k) % NZ
        pltpu.make_async_remote_copy(
            src_ref=rz.at[src], dst_ref=rz.at[src], send_sem=sz_s.at[src], recv_sem=sz_r.at[src],
            device_id=at(src, y, c), device_id_type=MESH,
        ).wait_recv()
        own = own + rz[src]
    pg_ref[...] = own[:, 0:D] * dinv[...]

    for cp in small_y + small_z:
        cp.wait_send()
    for t in range(4):
        core_copy(t).wait_send()
        for k in (1, 2, 3):
            x_copy(t, k).wait_send()
        for k in range(1, NY):
            y_copy(t, k).wait_send()
    for k in range(1, NZ):
        peer = (z + k) % NZ
        pltpu.make_async_remote_copy(
            src_ref=rz.at[peer], dst_ref=rz.at[peer], send_sem=sz_s.at[peer], recv_sem=sz_r.at[peer],
            device_id=at(peer, y, c), device_id_type=MESH,
        ).wait_send()


def hand_out(a, b, c, d, a_out, b_out, c_out, d_out, one, sem):
    one[...] = a[0:1, 0:1]
    pairs = ((d, d_out), (b, b_out), (c, c_out), (one, a_out))
    copies = [pltpu.make_async_copy(src, dst, sem.at[k]) for k, (src, dst) in enumerate(pairs)]
    for cp in copies:
        cp.start()
    for cp in copies:
        cp.wait()


def per_device(inner_noise, outer_noise, start, vol, times):
    K, D, M = inner_noise.shape
    hbm = pl.BlockSpec(memory_space=pltpu.HBM)
    vmem = pl.BlockSpec(memory_space=pltpu.VMEM)
    dma = pltpu.SemaphoreType.DMA
    V = pltpu.VMEM
    results = pl.pallas_call(
        kernel,
        out_shape=(V((1, 128), F32), V((1, D), F32), V((1, 8), F32), V((8, D), F32)),
        in_specs=[hbm] * 5,
        out_specs=(vmem,) * 4,
        scratch_shapes=[
            V((4, D, K, 128), BF16), V((D, M), BF16), V((1, D), F32), V((1, D), F32), V((1, M), F32),
            V((1, 256), F32), V((1, 256), F32), V((256, 128), F32), V((4, 256, 128), F32),
            V((4, K, 128), F32), V((3, 4, K, 128), F32), V((8, M), F32), V((256, 128), F32),
            V((4, NC, NY, 2, 8, 256), F32), V((4, NY, 2, 8, 256), F32),
            V((4, 3, 2, 8, 256), F32), V((NZ, 8, 256), F32),
            V((NY * NC, 8, 128), F32), V((NZ, 8, 128), F32), V((8, 128), F32),
            V((8, D), F32),
            dma((7 + 4 * CHUNKS,)), dma((12,)), dma((12,)), dma((4,)), dma((4,)), dma((12,)), dma((12,)),
            dma((NZ,)), dma((NZ,)), dma((7,)), dma((7,)), dma((7,)), dma((7,)),
            pltpu.SemaphoreType.REGULAR((6,)),
        ],
        compiler_params=pltpu.CompilerParams(
            collective_id=0, has_side_effects=True
        ),
    )(
        jnp.transpose(inner_noise, (1, 0, 2)), outer_noise, start[None], vol[None], times[None]
    )
    root_value, root_grad, point_value, point_grad = pl.pallas_call(
        hand_out,
        out_shape=tuple(jax.ShapeDtypeStruct(s, F32) for s in ((1, 1), (1, D), (1, 8), (8, D))),
        in_specs=[vmem] * 4,
        out_specs=(hbm,) * 4,
        scratch_shapes=[V((1, 1), F32), dma((4,))],
        compiler_params=pltpu.CompilerParams(vmem_limit_bytes=1024 * 1024),
    )(*results)
    return root_value[0], root_grad[0], point_value[0], point_grad.T


def solution(mesh):
    in_specs = (P("path", "dim", None), P("dim", None), P("dim"), P("dim"), P())
    out_specs = (P(), P("dim"), P("path"), P("dim", "path"))
    return jax.shard_map(
        per_device, mesh=mesh, in_specs=in_specs, out_specs=out_specs, check_vma=False
    )
```

```python
import functools

import jax
import jax.numpy as jnp
from jax import lax
from jax.experimental import pallas as pl
from jax.experimental.pallas import tpu as pltpu
from jax.sharding import PartitionSpec as P

drift = 0.02
delta = 2.0 / 3.0
rate_free = 0.02
gamma_high = 0.2
gamma_low = 0.02
value_high = 0.4
value_low = 0.7

NX, NY, NZ, NC = 4, 4, 8, 2
MESH = pl.DeviceIdType.MESH
F32 = jnp.float32
BF16 = jnp.bfloat16
CHUNKS = 5


def driver_of(value):
    slope = jnp.clip((value - value_high) / (value_low - value_high), 0.0, 1.0)
    quota = gamma_high + (gamma_low - gamma_high) * slope
    return -(1.0 - delta) * quota * value - rate_free * value


def smallest(terms):
    while len(terms) > 1:
        pairs = [jnp.minimum(a, b) for a, b in zip(terms[::2], terms[1::2])]
        terms = pairs + terms[len(pairs) * 2 :]
    return terms[0]


def kernel(
    noise_hbm, outer_hbm, start_hbm, vol_hbm, times_hbm,
    rv_ref, rg_ref, pv_ref, pg_ref,
    noise, turned, outer, start_v, vol_v, times_v,
    startp, volp, volb, abase, lmin, rx, rows_t, stage, nt, rc, ry, rz, rf, far_sum, bytes_of, smy, smz, tot, dinv,
    in_sem, sent, x_in, core_in, y_in, z_in, far_z_in, far_y_in, small_y_in, small_z_in, know,
):
    D, K, M = noise_hbm.shape
    path = lax.axis_index("path")
    x = lax.axis_index("dim")
    z = path // (NY * NC)
    y = (path // NC) % NY
    c = path % NC
    jz = z // 2

    def at_x(k):
        return (path, (x + k) % NX)

    def at(zz, yy, cc):
        return ((zz * NY + yy) * NC + cc, x)

    small_in = [
        pltpu.make_async_copy(vol_hbm, vol_v, in_sem.at[0]),
        pltpu.make_async_copy(start_hbm, start_v, in_sem.at[1]),
        pltpu.make_async_copy(times_hbm, times_v, in_sem.at[2]),
    ]
    for cp in small_in:
        cp.start()
    odd = z % 2
    blocks = [(jz + off) % 4 for off in (2, 1 + 2 * odd, 3 - 2 * odd, 0)]

    def lanes_of(t):
        return pl.ds(pl.multiple_of(blocks[t] * 128, 128), 128)

    per = D // CHUNKS
    outer_in = [
        pltpu.make_async_copy(outer_hbm.at[:, lanes_of(t)], outer.at[:, lanes_of(t)], in_sem.at[3 + t])
        for t in range(4)
    ]
    noise_in = [
        [
            pltpu.make_async_copy(
                noise_hbm.at[pl.ds(q * per, per), :, lanes_of(t)],
                noise.at[t, pl.ds(q * per, per)],
                in_sem.at[7 + t],
            )
            for q in range(CHUNKS)
        ]
        for t in range(4)
    ]
    for cp in [outer_in[0]] + noise_in[0]:
        cp.start()

    barrier = pltpu.get_barrier_semaphore()
    near = [at((z + k) % NZ, y, c) for k in (1, NZ - 1)]
    near += [at(z, (y + k) % NY, cc) for k in (1, NY - 1) for cc in (c, 1 - c)]
    near += [at_x(k) for k in (1, 2, 3)] + [at(z, y, 1 - c)]
    for peer in near:
        pl.semaphore_signal(barrier, inc=1, device_id=peer, device_id_type=MESH)

    def tell(sem, peer):
        pl.semaphore_signal(sem, inc=1, device_id=peer, device_id_type=MESH)

    z_next, z_last = at((z + 1) % NZ, y, c), at((z + NZ - 1) % NZ, y, c)

    for t in range(1, 4):
        for cp in [outer_in[t]] + noise_in[t]:
            cp.start()
    for t in range(4):
        noise[t, D:] = jnp.zeros((256 - D, K, 128), BF16)
    for cp in small_in:
        cp.wait()

    startp[...] = jnp.ones_like(startp)
    volp[...] = jnp.ones_like(volp)
    startp[:, 0:D] = start_v[...]
    volp[:, 0:D] = vol_v[...]
    vol = volp[...]
    begin = startp[...]
    times = times_v[...]
    tau = 1.0 - times
    root_t = jnp.sqrt(times)
    root_tau = jnp.sqrt(tau)
    inv_root_tau = 1.0 / root_tau
    offset = jnp.log(begin) + (drift - 0.5 * vol * vol)
    for h in range(2):
        volb[h * 128 : (h + 1) * 128, :] = jnp.broadcast_to(
            vol[:, h * 128 : (h + 1) * 128], (128, 128)
        ).T
        stage[h * 128 : (h + 1) * 128, :] = jnp.broadcast_to(
            offset[:, h * 128 : (h + 1) * 128], (128, 128)
        ).T
    rows_t[0:1, :] = root_t
    rows_t[1:2, :] = root_tau
    rows_t[2:3, :] = inv_root_tau

    def coefficients(t):
        outer_in[t].wait()
        scale = rows_t[0:1, lanes_of(t)]
        inv = rows_t[2:3, lanes_of(t)]
        for lo in range(0, D, 16):
            hi = min(lo + 16, D)
            o = outer[lo:hi, lanes_of(t)].astype(F32)
            abase[t, lo:hi, :] = (stage[lo:hi, :] + volb[lo:hi, :] * (scale * o)) * inv

    def arrived(ref, sem):
        pltpu.make_async_copy(ref, ref, sem).wait()

    def x_copy(t, k):
        return pltpu.make_async_remote_copy(
            src_ref=lmin.at[t], dst_ref=rx.at[t, k - 1], send_sem=sent, recv_sem=x_in.at[t],
            device_id=at_x(k), device_id_type=MESH,
        )

    def minimum_of(ts):
        for t in ts:
            here = noise.at[t, pl.ds(0, D)]
            pltpu.make_async_copy(here, here, in_sem.at[7 + t]).wait()
        acc = [jnp.full((K, 128), 3.0e38, F32) for _ in ts]
        for q in range(CHUNKS):
            terms = [[] for _ in ts]
            for d in range(q * per, (q + 1) * per):
                v = volb[pl.ds(d, K, stride=0), :]
                for row, t in zip(terms, ts):
                    row.append(noise[t, d].astype(F32) * v + abase[t, pl.ds(d, K, stride=0), :])
            acc = [jnp.minimum(a, smallest(r)) for a, r in zip(acc, terms)]
        for t, a in zip(ts, acc):
            lmin[t] = a

    for ts in ((0,), (1,), (2, 3)):
        for t in ts:
            coefficients(t)
        minimum_of(ts)
        if ts[0] == 0:
            pl.semaphore_wait(barrier, len(near))
            tell(know.at[0], at(z, (y + NY - 1) % NY, c))
            tell(know.at[1], z_last)
            tell(know.at[2], z_next)
        for t in ts:
            for k in (2, 1, 3):
                x_copy(t, k).start()

    lane = lax.broadcasted_iota(jnp.int32, (K, M), 1)
    row = lax.broadcasted_iota(jnp.int32, (K, M), 0)
    pick = lane == path * K + row
    own_t = jnp.sum(jnp.where(pick, times, 0.0), axis=1, keepdims=True)
    own_outer = lax.dot_general(
        jnp.where(pick, 1.0, 0.0).astype(BF16), outer[...], (((1,), (1,)), ((), ())),
        preferred_element_type=F32,
    )
    vol_d = vol_v[...]
    own_state = start_v[...] * jnp.exp(
        (drift - 0.5 * vol_d * vol_d) * own_t + vol_d * jnp.sqrt(own_t) * own_outer
    )
    dinv[...] = 1.0 / ((K * NZ * NY * NC) * vol_d * own_state * (1.0 - own_t))

    pl.semaphore_wait(know.at[0], 1)
    pl.semaphore_wait(know.at[1], 1)
    pl.semaphore_wait(know.at[2], 1)
    tell(know.at[3], z_last)
    tell(know.at[4], z_next)

    sub = lax.broadcasted_iota(jnp.int32, (8, 128), 0)

    def swapped(tiles, step):
        low = (sub & step) == 0
        out = list(tiles)
        for a in range(8):
            if a & step == 0:
                lo, hi = tiles[a], tiles[a + step]
                out[a] = jnp.where(low, lo, pltpu.roll(hi, step, axis=0))
                out[a + step] = jnp.where(low, pltpu.roll(lo, 8 - step, axis=0), hi)
        return out

    for t in range(4):

        def turn(r, _, t=t):
            for u in range(4):
                g = r * 4 + u
                tiles = [noise[t, g * 8 + s].astype(F32) for s in range(8)]
                for step in (4, 2, 1):
                    tiles = swapped(tiles, step)
                for k in range(8):
                    turned[t, k, pl.ds(pl.multiple_of(g * 8, 8), 8), :] = tiles[k]
            return 0

        lax.fori_loop(0, 8, turn, 0)

    pl.semaphore_wait(know.at[3], 1)
    pl.semaphore_wait(know.at[4], 1)
    tell(know.at[5], z_last)

    def core_copy(t):
        return pltpu.make_async_remote_copy(
            src_ref=nt.at[t, 1 - c], dst_ref=rc.at[t], send_sem=sent, recv_sem=core_in.at[t],
            device_id=at(z, y, 1 - c), device_id_type=MESH,
        )

    side = {1: 0, 3: 1}
    y_far = (y + 2) % NY

    def y_copy(t, k):
        peer = (y + k) % NY
        return pltpu.make_async_remote_copy(
            src_ref=nt.at[t, c, peer], dst_ref=ry.at[t, side[k]],
            send_sem=sent, recv_sem=y_in.at[t],
            device_id=at(z, peer, c), device_id_type=MESH,
        )

    def far_copy(t, peer, zz):
        return pltpu.make_async_remote_copy(
            src_ref=nt.at[t, c, y_far, zz], dst_ref=rf.at[z], send_sem=sent, recv_sem=far_z_in,
            device_id=at(peer, y, c), device_id_type=MESH,
        )

    def to_each(t, copy):
        if t == 3:
            copy(t, 2 * blocks[t] + 1 - odd, 1 - odd).start()
        else:
            for zz in range(2):
                copy(t, 2 * blocks[t] + zz, zz).start()

    def after_core(t):
        arrived(rc.at[t], core_in.at[t])
        nt[t, c] = nt[t, c] + rc[t]
        for k in (1, 3):
            y_copy(t, k).start()
        if t == 0:
            pl.semaphore_wait(know.at[5], 1)
        to_each(t, far_copy)

    wsum = [jnp.zeros((8, 128), F32)] * 2
    tot[...] = jnp.zeros_like(tot)
    for t, j in enumerate(blocks):
        arrived(rx.at[t], x_in.at[t])
        least = jnp.minimum(
            jnp.minimum(lmin[t], rx[t, 0]), jnp.minimum(rx[t, 1], rx[t, 2])
        )
        scale = rows_t[1:2, lanes_of(t)]
        payoff = jnp.exp(scale * least)
        p = payoff * scale
        tot[pl.ds(j, 1), :] = jnp.sum(payoff, axis=0, keepdims=True)
        rows = [jnp.broadcast_to(p[k : k + 1, :], (8, 128)) for k in range(K)]
        for h in range(2):
            tiles = []
            for g in range(16):
                first = h * 128 + g * 8
                terms = [turned[t, k, first : first + 8, :] * rows[k] for k in range(K)]
                while len(terms) > 1:
                    terms = [a + b for a, b in zip(terms[::2], terms[1::2])]
                tiles.append(terms[0])
            block = jnp.concatenate(tiles, axis=0).T
            part = jnp.zeros((8, 128), F32)
            for q in range(16):
                zz, yy, cc = q // 8, (q // 2) % 4, q % 2
                piece = block[q * 8 : (q + 1) * 8, :]
                nt[t, cc, yy, zz, :, h * 128 : (h + 1) * 128] = piece
                part = part + piece
            wsum[h] = wsum[h] + part
        if t == 3:
            for h in range(2):
                tot[4 + h : 5 + h, :] = jnp.sum(wsum[h], axis=0, keepdims=True)
            me = y * NC + c
            smy[me] = tot[...]
            for k in (4, 5, 3, 2, 7, 6, 1):
                cp = pltpu.make_async_remote_copy(
                    src_ref=smy.at[me], dst_ref=smy.at[me], send_sem=sent, recv_sem=small_y_in,
                    device_id=at(z, (y + k // 2) % NY, (c + k) % 2), device_id_type=MESH,
                )
                cp.start()
        core_copy(t).start()

    for t in range(3):
        after_core(t)
    after_core(3)

    def z_copy(t, peer, zz):
        return pltpu.make_async_remote_copy(
            src_ref=nt.at[t, c, y, zz], dst_ref=rz.at[z], send_sem=sent, recv_sem=z_in,
            device_id=at(peer, y, c), device_id_type=MESH,
        )

    def after_y(t):
        arrived(ry.at[t], y_in.at[t])
        nt[t, c, y] = nt[t, c, y] + (ry[t, 0] + ry[t, 1])
        to_each(t, z_copy)

    arrived(smy.at[pl.ds(0, NY * NC - 1)], small_y_in)
    smz[z] = ((smy[0] + smy[1]) + (smy[2] + smy[3])) + ((smy[4] + smy[5]) + (smy[6] + smy[7]))
    for k in (4, 3, 5, 2, 6, 1, 7):
        cp = pltpu.make_async_remote_copy(
            src_ref=smz.at[z], dst_ref=smz.at[z], send_sem=sent, recv_sem=small_z_in,
            device_id=at((z + k) % NZ, y, c), device_id_type=MESH,
        )
        cp.start()
    after_y(0)
    after_y(1)
    after_y(2)
    after_y(3)
    others = pl.ds(0, NZ - 1)
    arrived(rf.at[others], far_z_in)
    total = nt[3, c, y_far, odd]
    for k in range(1, NZ):
        src = (z + k) % NZ
        total = total + rf[src]
    far_sum[0] = total
    far_sent = pltpu.make_async_remote_copy(
        src_ref=far_sum.at[0], dst_ref=far_sum.at[1], send_sem=sent, recv_sem=far_y_in,
        device_id=at(z, y_far, c), device_id_type=MESH,
    )
    far_sent.start()

    arrived(smz.at[others], small_z_in)
    whole = ((smz[0] + smz[1]) + (smz[2] + smz[3])) + ((smz[4] + smz[5]) + (smz[6] + smz[7]))
    inner = K * NZ * NY * NC
    tot[...] = whole
    totals = jnp.concatenate([whole[k : k + 1, :] for k in range(4)], axis=1)
    driver = driver_of(totals * (1.0 / inner))
    rv_ref[...] = jnp.zeros((1, 128), F32) + (
        jnp.sum(totals, axis=1, keepdims=True) * (1.0 / (M * inner))
        + jnp.sum(driver, axis=1, keepdims=True) * (1.0 / M)
    )
    weight = root_t * totals * (1.0 / (M * inner)) + driver / (root_t * M)
    w_hi = weight.astype(BF16).astype(F32)
    w_mid = (weight - w_hi).astype(BF16).astype(F32)
    w_lo = weight - w_hi - w_mid
    rows = lax.broadcasted_iota(jnp.int32, (8, M), 0)
    lhs = jnp.where(rows == 0, w_hi, jnp.where(rows == 1, w_mid, jnp.where(rows == 2, w_lo, 0.0)))
    prod = lax.dot_general(
        lhs.astype(BF16), outer[...], (((1,), (1,)), ((), ())), preferred_element_type=F32
    )
    noise_sum = jnp.sum(prod, axis=0, keepdims=True)
    moment_sum = jnp.concatenate([whole[4:5, :], whole[5:6, :]], axis=1)[:, 0:D]
    rg_ref[...] = (noise_sum + moment_sum * (1.0 / (M * inner))) / (vol_v[...] * start_v[...])
    own_row = tot[pl.ds(path // 16, 1), :] * (1.0 / inner)
    own_row = pltpu.roll(jnp.broadcast_to(own_row, (8, 128)), (128 - (path % 16) * 8) % 128, axis=1)
    pv_ref[...] = own_row[0:1, 0:8]

    arrived(rz.at[others], z_in)
    own = nt[3, c, y, odd]
    for k in range(1, NZ):
        src = (z + k) % NZ
        own = own + rz[src]
    far_sent.wait_recv()
    own = own + far_sum[1]
    pg_ref[...] = own[:, 0:D] * dinv[...]

    rows_sent = 4 * 3 * 8 + 4 * 128 + 4 * 2 * 32 + 2 * 7 * 16 + 2 * 7 * 8 + 16
    arrived(bytes_of.at[pl.ds(0, rows_sent)], sent)


def hand_out(a, b, c, d, a_out, b_out, c_out, d_out, one, sem):
    one[...] = a[0:1, 0:1]
    pairs = ((d, d_out), (b, b_out), (c, c_out), (one, a_out))
    copies = [pltpu.make_async_copy(src, dst, sem.at[k]) for k, (src, dst) in enumerate(pairs)]
    for cp in copies:
        cp.start()
    for cp in copies:
        cp.wait()


def per_device(inner_noise, outer_noise, start, vol, times):
    K, D, M = inner_noise.shape
    hbm = pl.BlockSpec(memory_space=pltpu.HBM)
    vmem = pl.BlockSpec(memory_space=pltpu.VMEM)
    dma = pltpu.SemaphoreType.DMA
    V = pltpu.VMEM
    results = pl.pallas_call(
        kernel,
        out_shape=(V((1, 128), F32), V((1, D), F32), V((1, 8), F32), V((8, D), F32)),
        in_specs=[hbm] * 5,
        out_specs=(vmem,) * 4,
        scratch_shapes=[
            V((4, 256, K, 128), BF16), V((4, K, 256, 128), F32), V((D, M), BF16), V((1, D), F32), V((1, D), F32), V((1, M), F32),
            V((1, 256), F32), V((1, 256), F32), V((256, 128), F32), V((4, 256, 128), F32),
            V((4, K, 128), F32), V((4, 3, K, 128), F32), V((8, M), F32), V((256, 128), F32),
            V((4, NC, NY, 2, 8, 256), F32), V((4, NY, 2, 8, 256), F32),
            V((4, 2, 2, 8, 256), F32), V((NZ, 8, 256), F32), V((NZ, 8, 256), F32), V((2, 8, 256), F32), V((1216, 128), F32),
            V((NY * NC, 8, 128), F32), V((NZ, 8, 128), F32), V((8, 128), F32),
            V((8, D), F32),
            dma((11,)), dma, dma((4,)), dma((4,)), dma((4,)), dma, dma, dma, dma, dma,
            pltpu.SemaphoreType.REGULAR((6,)),
        ],
        compiler_params=pltpu.CompilerParams(
            collective_id=0, has_side_effects=True
        ),
    )(
        jnp.transpose(inner_noise, (1, 0, 2)), outer_noise, start[None], vol[None], times[None]
    )
    root_value, root_grad, point_value, point_grad = pl.pallas_call(
        hand_out,
        out_shape=tuple(jax.ShapeDtypeStruct(s, F32) for s in ((1, 1), (1, D), (1, 8), (8, D))),
        in_specs=[vmem] * 4,
        out_specs=(hbm,) * 4,
        scratch_shapes=[V((1, 1), F32), dma((4,))],
        compiler_params=pltpu.CompilerParams(vmem_limit_bytes=1024 * 1024),
    )(*results)
    return root_value[0], root_grad[0], point_value[0], point_grad.T


def solution(mesh):
    in_specs = (P("path", "dim", None), P("dim", None), P("dim"), P("dim"), P())
    out_specs = (P(), P("dim"), P("path"), P("dim", "path"))
    return jax.shard_map(
        per_device, mesh=mesh, in_specs=in_specs, out_specs=out_specs, check_vma=False
    )
```

```python
import functools

import jax
import jax.numpy as jnp
from jax import lax
from jax.experimental import pallas as pl
from jax.experimental.pallas import tpu as pltpu
from jax.sharding import PartitionSpec as P

drift = 0.02
delta = 2.0 / 3.0
rate_free = 0.02
gamma_high = 0.2
gamma_low = 0.02
value_high = 0.4
value_low = 0.7

NX, NY, NZ, NC = 4, 4, 8, 2
MESH = pl.DeviceIdType.MESH
F32 = jnp.float32
BF16 = jnp.bfloat16
CHUNKS = 5


def driver_of(value):
    slope = jnp.clip((value - value_high) / (value_low - value_high), 0.0, 1.0)
    quota = gamma_high + (gamma_low - gamma_high) * slope
    return -(1.0 - delta) * quota * value - rate_free * value


def smallest(terms):
    while len(terms) > 1:
        pairs = [jnp.minimum(a, b) for a, b in zip(terms[::2], terms[1::2])]
        terms = pairs + terms[len(pairs) * 2 :]
    return terms[0]


def kernel(
    noise_hbm, outer_hbm, start_hbm, vol_hbm, times_hbm,
    rv_ref, rg_ref, pv_ref, pg_ref,
    noise, turned, outer, start_v, vol_v, times_v,
    startp, volp, volb, abase, lmin, rx, rows_t, stage, nt, rc, ry, rz, rf, far_sum, bytes_of, smy, smz, tot, dinv,
    in_sem, sent, x_in, core_in, y_in, z_in, far_z_in, far_y_in, small_y_in, small_z_in, know,
):
    D, K, M = noise_hbm.shape
    path = lax.axis_index("path")
    x = lax.axis_index("dim")
    z = path // (NY * NC)
    y = (path // NC) % NY
    c = path % NC
    jz = z // 2

    def at_x(k):
        return (path, (x + k) % NX)

    def at(zz, yy, cc):
        return ((zz * NY + yy) * NC + cc, x)

    small_in = [
        pltpu.make_async_copy(vol_hbm, vol_v, in_sem.at[0]),
        pltpu.make_async_copy(start_hbm, start_v, in_sem.at[1]),
        pltpu.make_async_copy(times_hbm, times_v, in_sem.at[2]),
    ]
    for cp in small_in:
        cp.start()
    odd = z % 2
    blocks = [(jz + off) % 4 for off in (2, 1 + 2 * odd, 3 - 2 * odd, 0)]

    def lanes_of(t):
        return pl.ds(pl.multiple_of(blocks[t] * 128, 128), 128)

    per = D // CHUNKS
    noise_in = [
        [
            pltpu.make_async_copy(
                noise_hbm.at[pl.ds(q * per, per), :, lanes_of(t)],
                noise.at[t, pl.ds(q * per, per)],
                in_sem.at[4 + t],
            )
            for q in range(CHUNKS)
        ]
        for t in range(4)
    ]
    outer_in = pltpu.make_async_copy(outer_hbm, outer, in_sem.at[3])
    outer_in.start()
    for cp in noise_in[0]:
        cp.start()

    barrier = pltpu.get_barrier_semaphore()
    near = [at((z + k) % NZ, y, c) for k in (1, NZ - 1)]
    near += [at(z, (y + k) % NY, cc) for k in (1, NY - 1) for cc in (c, 1 - c)]
    near += [at_x(k) for k in (1, 2, 3)] + [at(z, y, 1 - c)]
    for peer in near:
        pl.semaphore_signal(barrier, inc=1, device_id=peer, device_id_type=MESH)

    def tell(sem, peer):
        pl.semaphore_signal(sem, inc=1, device_id=peer, device_id_type=MESH)

    z_next, z_last = at((z + 1) % NZ, y, c), at((z + NZ - 1) % NZ, y, c)

    for t in range(1, 4):
        for cp in noise_in[t]:
            cp.start()
    for t in range(4):
        noise[t, D:] = jnp.zeros((256 - D, K, 128), BF16)
    for cp in small_in:
        cp.wait()

    startp[...] = jnp.ones_like(startp)
    volp[...] = jnp.ones_like(volp)
    startp[:, 0:D] = start_v[...]
    volp[:, 0:D] = vol_v[...]
    vol = volp[...]
    begin = startp[...]
    times = times_v[...]
    tau = 1.0 - times
    root_t = jnp.sqrt(times)
    root_tau = jnp.sqrt(tau)
    inv_root_tau = 1.0 / root_tau
    offset = jnp.log(begin) + (drift - 0.5 * vol * vol)
    for h in range(2):
        volb[h * 128 : (h + 1) * 128, :] = jnp.broadcast_to(
            vol[:, h * 128 : (h + 1) * 128], (128, 128)
        ).T
        stage[h * 128 : (h + 1) * 128, :] = jnp.broadcast_to(
            offset[:, h * 128 : (h + 1) * 128], (128, 128)
        ).T
    rows_t[0:1, :] = root_t
    rows_t[1:2, :] = root_tau
    rows_t[2:3, :] = inv_root_tau

    def coefficients(t):
        scale = rows_t[0:1, lanes_of(t)]
        inv = rows_t[2:3, lanes_of(t)]
        for lo in range(0, D, 16):
            hi = min(lo + 16, D)
            o = outer[lo:hi, lanes_of(t)].astype(F32)
            abase[t, lo:hi, :] = (stage[lo:hi, :] + volb[lo:hi, :] * (scale * o)) * inv

    def arrived(ref, sem):
        pltpu.make_async_copy(ref, ref, sem).wait()

    def x_copy(t, k):
        return pltpu.make_async_remote_copy(
            src_ref=lmin.at[t], dst_ref=rx.at[t, k - 1], send_sem=sent, recv_sem=x_in.at[t],
            device_id=at_x(k), device_id_type=MESH,
        )

    def minimum_of(ts):
        for t in ts:
            here = noise.at[t, pl.ds(0, D)]
            pltpu.make_async_copy(here, here, in_sem.at[4 + t]).wait()
        acc = [jnp.full((K, 128), 3.0e38, F32) for _ in ts]
        for q in range(CHUNKS):
            terms = [[] for _ in ts]
            for d in range(q * per, (q + 1) * per):
                v = volb[pl.ds(d, K, stride=0), :]
                for row, t in zip(terms, ts):
                    row.append(noise[t, d].astype(F32) * v + abase[t, pl.ds(d, K, stride=0), :])
            acc = [jnp.minimum(a, smallest(r)) for a, r in zip(acc, terms)]
        for t, a in zip(ts, acc):
            lmin[t] = a

    outer_in.wait()
    for t in range(4):
        coefficients(t)
    for ts in ((0,), (1,), (2, 3)):
        minimum_of(ts)
        if ts[0] == 0:
            pl.semaphore_wait(barrier, len(near))
            tell(know.at[0], at(z, (y + NY - 1) % NY, c))
            tell(know.at[1], z_last)
            tell(know.at[2], z_next)
        for t in ts:
            for k in (2, 1, 3):
                x_copy(t, k).start()

    lane = lax.broadcasted_iota(jnp.int32, (K, M), 1)
    row = lax.broadcasted_iota(jnp.int32, (K, M), 0)
    pick = lane == path * K + row
    own_t = jnp.sum(jnp.where(pick, times, 0.0), axis=1, keepdims=True)
    own_outer = lax.dot_general(
        jnp.where(pick, 1.0, 0.0).astype(BF16), outer[...], (((1,), (1,)), ((), ())),
        preferred_element_type=F32,
    )
    vol_d = vol_v[...]
    own_state = start_v[...] * jnp.exp(
        (drift - 0.5 * vol_d * vol_d) * own_t + vol_d * jnp.sqrt(own_t) * own_outer
    )
    dinv[...] = 1.0 / ((K * NZ * NY * NC) * vol_d * own_state * (1.0 - own_t))

    pl.semaphore_wait(know.at[0], 1)
    pl.semaphore_wait(know.at[1], 1)
    pl.semaphore_wait(know.at[2], 1)
    tell(know.at[3], z_last)
    tell(know.at[4], z_next)

    sub = lax.broadcasted_iota(jnp.int32, (8, 128), 0)

    def swapped(tiles, step):
        low = (sub & step) == 0
        out = list(tiles)
        for a in range(8):
            if a & step == 0:
                lo, hi = tiles[a], tiles[a + step]
                out[a] = jnp.where(low, lo, pltpu.roll(hi, step, axis=0))
                out[a + step] = jnp.where(low, pltpu.roll(lo, 8 - step, axis=0), hi)
        return out

    for t in range(4):

        def turn(r, _, t=t):
            for u in range(4):
                g = r * 4 + u
                tiles = [noise[t, g * 8 + s].astype(F32) for s in range(8)]
                for step in (4, 2, 1):
                    tiles = swapped(tiles, step)
                for k in range(8):
                    turned[t, k, pl.ds(pl.multiple_of(g * 8, 8), 8), :] = tiles[k]
            return 0

        lax.fori_loop(0, 8, turn, 0)

    def core_copy(t):
        return pltpu.make_async_remote_copy(
            src_ref=nt.at[t, 1 - c], dst_ref=rc.at[t], send_sem=sent, recv_sem=core_in.at[t],
            device_id=at(z, y, 1 - c), device_id_type=MESH,
        )

    side = {1: 0, 3: 1}
    y_far = (y + 2) % NY

    def y_copy(t, k):
        peer = (y + k) % NY
        return pltpu.make_async_remote_copy(
            src_ref=nt.at[t, c, peer], dst_ref=ry.at[t, side[k]],
            send_sem=sent, recv_sem=y_in.at[t],
            device_id=at(z, peer, c), device_id_type=MESH,
        )

    def far_copy(t, peer, zz):
        return pltpu.make_async_remote_copy(
            src_ref=nt.at[t, c, y_far, zz], dst_ref=rf.at[z], send_sem=sent, recv_sem=far_z_in,
            device_id=at(peer, y, c), device_id_type=MESH,
        )

    def to_each(t, copy):
        if t == 3:
            copy(t, 2 * blocks[t] + 1 - odd, 1 - odd).start()
        else:
            for zz in range(2):
                copy(t, 2 * blocks[t] + zz, zz).start()

    def after_core(t):
        arrived(rc.at[t], core_in.at[t])
        nt[t, c] = nt[t, c] + rc[t]
        if t == 0:
            pl.semaphore_wait(know.at[5], 1)
        to_each(t, far_copy)
        for k in (1, 3):
            y_copy(t, k).start()

    wsum = [jnp.zeros((8, 128), F32)] * 2
    tot[...] = jnp.zeros_like(tot)
    for t, j in enumerate(blocks):
        arrived(rx.at[t], x_in.at[t])
        least = jnp.minimum(
            jnp.minimum(lmin[t], rx[t, 0]), jnp.minimum(rx[t, 1], rx[t, 2])
        )
        scale = rows_t[1:2, lanes_of(t)]
        payoff = jnp.exp(scale * least)
        p = payoff * scale
        tot[pl.ds(j, 1), :] = jnp.sum(payoff, axis=0, keepdims=True)
        rows = [jnp.broadcast_to(p[k : k + 1, :], (8, 128)) for k in range(K)]
        for h in range(2):
            tiles = []
            for g in range(16):
                first = h * 128 + g * 8
                terms = [turned[t, k, first : first + 8, :] * rows[k] for k in range(K)]
                while len(terms) > 1:
                    terms = [a + b for a, b in zip(terms[::2], terms[1::2])]
                tiles.append(terms[0])
            block = jnp.concatenate(tiles, axis=0).T
            part = jnp.zeros((8, 128), F32)
            for q in range(16):
                zz, yy, cc = q // 8, (q // 2) % 4, q % 2
                piece = block[q * 8 : (q + 1) * 8, :]
                nt[t, cc, yy, zz, :, h * 128 : (h + 1) * 128] = piece
                part = part + piece
            wsum[h] = wsum[h] + part
        if t == 3:
            for h in range(2):
                tot[4 + h : 5 + h, :] = jnp.sum(wsum[h], axis=0, keepdims=True)
            me = y * NC + c
            smy[me] = tot[...]
            for k in (4, 5, 3, 2, 7, 6, 1):
                cp = pltpu.make_async_remote_copy(
                    src_ref=smy.at[me], dst_ref=smy.at[me], send_sem=sent, recv_sem=small_y_in,
                    device_id=at(z, (y + k // 2) % NY, (c + k) % 2), device_id_type=MESH,
                )
                cp.start()
        core_copy(t).start()
        if t == 1:
            pl.semaphore_wait(know.at[3], 1)
            pl.semaphore_wait(know.at[4], 1)
            tell(know.at[5], z_last)

    for t in range(3):
        after_core(t)
    after_core(3)

    def z_copy(t, peer, zz):
        return pltpu.make_async_remote_copy(
            src_ref=nt.at[t, c, y, zz], dst_ref=rz.at[z], send_sem=sent, recv_sem=z_in,
            device_id=at(peer, y, c), device_id_type=MESH,
        )

    def after_y(t):
        arrived(ry.at[t], y_in.at[t])
        nt[t, c, y] = nt[t, c, y] + (ry[t, 0] + ry[t, 1])
        to_each(t, z_copy)

    arrived(smy.at[pl.ds(0, NY * NC - 1)], small_y_in)
    smz[z] = ((smy[0] + smy[1]) + (smy[2] + smy[3])) + ((smy[4] + smy[5]) + (smy[6] + smy[7]))
    for k in (4, 3, 5, 2, 6, 1, 7):
        cp = pltpu.make_async_remote_copy(
            src_ref=smz.at[z], dst_ref=smz.at[z], send_sem=sent, recv_sem=small_z_in,
            device_id=at((z + k) % NZ, y, c), device_id_type=MESH,
        )
        cp.start()
    after_y(0)
    after_y(1)
    after_y(2)
    after_y(3)
    others = pl.ds(0, NZ - 1)
    arrived(rf.at[others], far_z_in)
    total = nt[3, c, y_far, odd]
    for k in range(1, NZ):
        src = (z + k) % NZ
        total = total + rf[src]
    far_sum[0] = total
    far_sent = pltpu.make_async_remote_copy(
        src_ref=far_sum.at[0], dst_ref=far_sum.at[1], send_sem=sent, recv_sem=far_y_in,
        device_id=at(z, y_far, c), device_id_type=MESH,
    )
    far_sent.start()

    arrived(smz.at[others], small_z_in)
    whole = ((smz[0] + smz[1]) + (smz[2] + smz[3])) + ((smz[4] + smz[5]) + (smz[6] + smz[7]))
    inner = K * NZ * NY * NC
    tot[...] = whole
    totals = jnp.concatenate([whole[k : k + 1, :] for k in range(4)], axis=1)
    driver = driver_of(totals * (1.0 / inner))
    rv_ref[...] = jnp.zeros((1, 128), F32) + (
        jnp.sum(totals, axis=1, keepdims=True) * (1.0 / (M * inner))
        + jnp.sum(driver, axis=1, keepdims=True) * (1.0 / M)
    )
    weight = root_t * totals * (1.0 / (M * inner)) + driver / (root_t * M)
    w_hi = weight.astype(BF16).astype(F32)
    w_mid = (weight - w_hi).astype(BF16).astype(F32)
    w_lo = weight - w_hi - w_mid
    rows = lax.broadcasted_iota(jnp.int32, (8, M), 0)
    lhs = jnp.where(rows == 0, w_hi, jnp.where(rows == 1, w_mid, jnp.where(rows == 2, w_lo, 0.0)))
    prod = lax.dot_general(
        lhs.astype(BF16), outer[...], (((1,), (1,)), ((), ())), preferred_element_type=F32
    )
    noise_sum = jnp.sum(prod, axis=0, keepdims=True)
    moment_sum = jnp.concatenate([whole[4:5, :], whole[5:6, :]], axis=1)[:, 0:D]
    rg_ref[...] = (noise_sum + moment_sum * (1.0 / (M * inner))) / (vol_v[...] * start_v[...])
    own_row = tot[pl.ds(path // 16, 1), :] * (1.0 / inner)
    own_row = pltpu.roll(jnp.broadcast_to(own_row, (8, 128)), (128 - (path % 16) * 8) % 128, axis=1)
    pv_ref[...] = own_row[0:1, 0:8]

    arrived(rz.at[others], z_in)
    own = nt[3, c, y, odd]
    for k in range(1, NZ):
        src = (z + k) % NZ
        own = own + rz[src]
    far_sent.wait_recv()
    own = own + far_sum[1]
    pg_ref[...] = own[:, 0:D] * dinv[...]

    rows_sent = 4 * 3 * 8 + 4 * 128 + 4 * 2 * 32 + 2 * 7 * 16 + 2 * 7 * 8 + 16
    arrived(bytes_of.at[pl.ds(0, rows_sent)], sent)


def hand_out(a, b, c, d, a_out, b_out, c_out, d_out, one, sem):
    one[...] = a[0:1, 0:1]
    pairs = ((d, d_out), (b, b_out), (c, c_out), (one, a_out))
    copies = [pltpu.make_async_copy(src, dst, sem.at[k]) for k, (src, dst) in enumerate(pairs)]
    for cp in copies:
        cp.start()
    for cp in copies:
        cp.wait()


def per_device(inner_noise, outer_noise, start, vol, times):
    K, D, M = inner_noise.shape
    hbm = pl.BlockSpec(memory_space=pltpu.HBM)
    vmem = pl.BlockSpec(memory_space=pltpu.VMEM)
    dma = pltpu.SemaphoreType.DMA
    V = pltpu.VMEM
    results = pl.pallas_call(
        kernel,
        out_shape=(V((1, 128), F32), V((1, D), F32), V((1, 8), F32), V((8, D), F32)),
        in_specs=[hbm] * 5,
        out_specs=(vmem,) * 4,
        scratch_shapes=[
            V((4, 256, K, 128), BF16), V((4, K, 256, 128), F32), V((D, M), BF16), V((1, D), F32), V((1, D), F32), V((1, M), F32),
            V((1, 256), F32), V((1, 256), F32), V((256, 128), F32), V((4, 256, 128), F32),
            V((4, K, 128), F32), V((4, 3, K, 128), F32), V((8, M), F32), V((256, 128), F32),
            V((4, NC, NY, 2, 8, 256), F32), V((4, NY, 2, 8, 256), F32),
            V((4, 2, 2, 8, 256), F32), V((NZ, 8, 256), F32), V((NZ, 8, 256), F32), V((2, 8, 256), F32), V((1216, 128), F32),
            V((NY * NC, 8, 128), F32), V((NZ, 8, 128), F32), V((8, 128), F32),
            V((8, D), F32),
            dma((8,)), dma, dma((4,)), dma((4,)), dma((4,)), dma, dma, dma, dma, dma,
            pltpu.SemaphoreType.REGULAR((6,)),
        ],
        compiler_params=pltpu.CompilerParams(
            collective_id=0, has_side_effects=True
        ),
    )(
        jnp.transpose(inner_noise, (1, 0, 2)), outer_noise, start[None], vol[None], times[None]
    )
    root_value, root_grad, point_value, point_grad = pl.pallas_call(
        hand_out,
        out_shape=tuple(jax.ShapeDtypeStruct(s, F32) for s in ((1, 1), (1, D), (1, 8), (8, D))),
        in_specs=[vmem] * 4,
        out_specs=(hbm,) * 4,
        scratch_shapes=[V((1, 1), F32), dma((4,))],
        compiler_params=pltpu.CompilerParams(vmem_limit_bytes=1024 * 1024),
    )(*results)
    return root_value[0], root_grad[0], point_value[0], point_grad.T


def solution(mesh):
    in_specs = (P("path", "dim", None), P("dim", None), P("dim"), P("dim"), P())
    out_specs = (P(), P("dim"), P("path"), P("dim", "path"))
    return jax.shard_map(
        per_device, mesh=mesh, in_specs=in_specs, out_specs=out_specs, check_vma=False
    )
```

```python
import functools

import jax
import jax.numpy as jnp
from jax import lax
from jax.experimental import pallas as pl
from jax.experimental.pallas import tpu as pltpu
from jax.sharding import PartitionSpec as P

drift = 0.02
delta = 2.0 / 3.0
rate_free = 0.02
gamma_high = 0.2
gamma_low = 0.02
value_high = 0.4
value_low = 0.7

NX, NY, NZ, NC = 4, 4, 8, 2
MESH = pl.DeviceIdType.MESH
F32 = jnp.float32
BF16 = jnp.bfloat16
CHUNKS = 5


def driver_of(value):
    slope = jnp.clip((value - value_high) / (value_low - value_high), 0.0, 1.0)
    quota = gamma_high + (gamma_low - gamma_high) * slope
    return -(1.0 - delta) * quota * value - rate_free * value


def smallest(terms):
    while len(terms) > 1:
        pairs = [jnp.minimum(a, b) for a, b in zip(terms[::2], terms[1::2])]
        terms = pairs + terms[len(pairs) * 2 :]
    return terms[0]


def kernel(
    noise_hbm, outer_hbm, start_hbm, vol_hbm, times_hbm,
    rv_ref, rg_ref, pv_ref, pg_ref,
    noise, turned, outer, start_v, vol_v, times_v,
    startp, volp, volb, abase, lmin, rx, rows_t, stage, nt, rc, ry, rz, rf, far_sum, bytes_of, smy, smz, tot, dinv,
    in_sem, sent, x_in, core_in, y_in, z_in, far_z_in, far_y_in, small_y_in, small_z_in, know,
):
    D, K, M = noise_hbm.shape
    path = lax.axis_index("path")
    x = lax.axis_index("dim")
    z = path // (NY * NC)
    y = (path // NC) % NY
    c = path % NC
    jz = z // 2

    def at_x(k):
        return (path, (x + k) % NX)

    def at(zz, yy, cc):
        return ((zz * NY + yy) * NC + cc, x)

    small_in = [
        pltpu.make_async_copy(vol_hbm, vol_v, in_sem.at[0]),
        pltpu.make_async_copy(start_hbm, start_v, in_sem.at[1]),
        pltpu.make_async_copy(times_hbm, times_v, in_sem.at[2]),
    ]
    for cp in small_in:
        cp.start()
    odd = z % 2
    blocks = [(jz + off) % 4 for off in (2, 1 + 2 * odd, 3 - 2 * odd, 0)]

    def lanes_of(t):
        return pl.ds(pl.multiple_of(blocks[t] * 128, 128), 128)

    per = D // CHUNKS
    noise_in = [
        [
            pltpu.make_async_copy(
                noise_hbm.at[pl.ds(q * per, per), :, lanes_of(t)],
                noise.at[t, pl.ds(q * per, per)],
                in_sem.at[4 + t],
            )
            for q in range(CHUNKS)
        ]
        for t in range(4)
    ]
    outer_in = pltpu.make_async_copy(outer_hbm, outer, in_sem.at[3])
    outer_in.start()
    for cp in noise_in[0]:
        cp.start()

    barrier = pltpu.get_barrier_semaphore()
    near = [at((z + k) % NZ, y, c) for k in (1, NZ - 1)]
    near += [at(z, (y + k) % NY, cc) for k in (1, NY - 1) for cc in (c, 1 - c)]
    near += [at_x(k) for k in (1, 2, 3)] + [at(z, y, 1 - c)]
    for peer in near:
        pl.semaphore_signal(barrier, inc=1, device_id=peer, device_id_type=MESH)

    def tell(sem, peer):
        pl.semaphore_signal(sem, inc=1, device_id=peer, device_id_type=MESH)

    z_next, z_last = at((z + 1) % NZ, y, c), at((z + NZ - 1) % NZ, y, c)

    for t in range(1, 4):
        for cp in noise_in[t]:
            cp.start()
    for t in range(4):
        noise[t, D:] = jnp.zeros((256 - D, K, 128), BF16)
    for cp in small_in:
        cp.wait()

    startp[...] = jnp.ones_like(startp)
    volp[...] = jnp.ones_like(volp)
    startp[:, 0:D] = start_v[...]
    volp[:, 0:D] = vol_v[...]
    vol = volp[...]
    begin = startp[...]
    times = times_v[...]
    tau = 1.0 - times
    root_t = jnp.sqrt(times)
    root_tau = jnp.sqrt(tau)
    inv_root_tau = 1.0 / root_tau
    offset = jnp.log(begin) + (drift - 0.5 * vol * vol)
    for h in range(2):
        volb[h * 128 : (h + 1) * 128, :] = jnp.broadcast_to(
            vol[:, h * 128 : (h + 1) * 128], (128, 128)
        ).T
        stage[h * 128 : (h + 1) * 128, :] = jnp.broadcast_to(
            offset[:, h * 128 : (h + 1) * 128], (128, 128)
        ).T
    rows_t[0:1, :] = root_t
    rows_t[1:2, :] = root_tau
    rows_t[2:3, :] = inv_root_tau

    def coefficients(t):
        scale = rows_t[0:1, lanes_of(t)]
        inv = rows_t[2:3, lanes_of(t)]
        for lo in range(0, D, 16):
            hi = min(lo + 16, D)
            o = outer[lo:hi, lanes_of(t)].astype(F32)
            abase[t, lo:hi, :] = (stage[lo:hi, :] + volb[lo:hi, :] * (scale * o)) * inv

    def arrived(ref, sem):
        pltpu.make_async_copy(ref, ref, sem).wait()

    def x_copy(t, k):
        return pltpu.make_async_remote_copy(
            src_ref=lmin.at[t], dst_ref=rx.at[t, k - 1], send_sem=sent, recv_sem=x_in.at[t],
            device_id=at_x(k), device_id_type=MESH,
        )

    def minimum_of(ts):
        for t in ts:
            here = noise.at[t, pl.ds(0, D)]
            pltpu.make_async_copy(here, here, in_sem.at[4 + t]).wait()
        acc = [jnp.full((K, 128), 3.0e38, F32) for _ in ts]
        for q in range(CHUNKS):
            terms = [[] for _ in ts]
            for d in range(q * per, (q + 1) * per):
                v = volb[pl.ds(d, K, stride=0), :]
                for row, t in zip(terms, ts):
                    row.append(noise[t, d].astype(F32) * v + abase[t, pl.ds(d, K, stride=0), :])
            acc = [jnp.minimum(a, smallest(r)) for a, r in zip(acc, terms)]
        for t, a in zip(ts, acc):
            lmin[t] = a

    outer_in.wait()
    for t in range(4):
        coefficients(t)
    for ts in ((0,), (1,), (2, 3)):
        minimum_of(ts)
        if ts[0] == 0:
            pl.semaphore_wait(barrier, len(near))
            tell(know.at[0], at(z, (y + NY - 1) % NY, c))
            tell(know.at[1], z_last)
            tell(know.at[2], z_next)
        for t in ts:
            for k in (2, 1, 3):
                x_copy(t, k).start()

    lane = lax.broadcasted_iota(jnp.int32, (K, M), 1)
    row = lax.broadcasted_iota(jnp.int32, (K, M), 0)
    pick = lane == path * K + row
    own_t = jnp.sum(jnp.where(pick, times, 0.0), axis=1, keepdims=True)
    own_outer = lax.dot_general(
        jnp.where(pick, 1.0, 0.0).astype(BF16), outer[...], (((1,), (1,)), ((), ())),
        preferred_element_type=F32,
    )
    vol_d = vol_v[...]
    own_state = start_v[...] * jnp.exp(
        (drift - 0.5 * vol_d * vol_d) * own_t + vol_d * jnp.sqrt(own_t) * own_outer
    )
    dinv[...] = 1.0 / ((K * NZ * NY * NC) * vol_d * own_state * (1.0 - own_t))

    pl.semaphore_wait(know.at[0], 1)
    pl.semaphore_wait(know.at[1], 1)
    pl.semaphore_wait(know.at[2], 1)
    tell(know.at[3], z_last)
    tell(know.at[4], z_next)

    sub = lax.broadcasted_iota(jnp.int32, (8, 128), 0)

    def swapped(tiles, step):
        low = (sub & step) == 0
        out = list(tiles)
        for a in range(8):
            if a & step == 0:
                lo, hi = tiles[a], tiles[a + step]
                out[a] = jnp.where(low, lo, pltpu.roll(hi, step, axis=0))
                out[a + step] = jnp.where(low, pltpu.roll(lo, 8 - step, axis=0), hi)
        return out

    for t in range(4):

        def turn(r, _, t=t):
            for u in range(4):
                g = r * 4 + u
                tiles = [noise[t, g * 8 + s].astype(F32) for s in range(8)]
                for step in (4, 2, 1):
                    tiles = swapped(tiles, step)
                for k in range(8):
                    turned[t, k, pl.ds(pl.multiple_of(g * 8, 8), 8), :] = tiles[k]
            return 0

        lax.fori_loop(0, 8, turn, 0)

    def core_copy(t):
        return pltpu.make_async_remote_copy(
            src_ref=nt.at[t, 1 - c], dst_ref=rc.at[t], send_sem=sent, recv_sem=core_in.at[t],
            device_id=at(z, y, 1 - c), device_id_type=MESH,
        )

    side = {1: 0, 3: 1}
    y_far = (y + 2) % NY

    def y_copy(t, k):
        peer = (y + k) % NY
        return pltpu.make_async_remote_copy(
            src_ref=nt.at[t, c, peer], dst_ref=ry.at[t, side[k]],
            send_sem=sent, recv_sem=y_in.at[t],
            device_id=at(z, peer, c), device_id_type=MESH,
        )

    def far_copy(t, peer, zz):
        return pltpu.make_async_remote_copy(
            src_ref=nt.at[t, c, y_far, zz], dst_ref=rf.at[z], send_sem=sent, recv_sem=far_z_in,
            device_id=at(peer, y, c), device_id_type=MESH,
        )

    def to_each(t, copy):
        if t == 3:
            copy(t, 2 * blocks[t] + 1 - odd, 1 - odd).start()
        else:
            for zz in range(2):
                copy(t, 2 * blocks[t] + zz, zz).start()

    def after_core(t):
        arrived(rc.at[t], core_in.at[t])
        nt[t, c] = nt[t, c] + rc[t]
        if t == 0:
            pl.semaphore_wait(know.at[5], 1)
        to_each(t, far_copy)
        for k in (1, 3):
            y_copy(t, k).start()

    wsum = [jnp.zeros((8, 128), F32)] * 2
    tot[...] = jnp.zeros_like(tot)
    for t, j in enumerate(blocks):
        arrived(rx.at[t], x_in.at[t])
        least = jnp.minimum(
            jnp.minimum(lmin[t], rx[t, 0]), jnp.minimum(rx[t, 1], rx[t, 2])
        )
        scale = rows_t[1:2, lanes_of(t)]
        payoff = jnp.exp(scale * least)
        p = payoff * scale
        tot[pl.ds(j, 1), :] = jnp.sum(payoff, axis=0, keepdims=True)
        rows = [jnp.broadcast_to(p[k : k + 1, :], (8, 128)) for k in range(K)]
        for h in range(2):
            tiles = []
            for g in range(16):
                first = h * 128 + g * 8
                terms = [turned[t, k, first : first + 8, :] * rows[k] for k in range(K)]
                while len(terms) > 1:
                    terms = [a + b for a, b in zip(terms[::2], terms[1::2])]
                tiles.append(terms[0])
            block = jnp.concatenate(tiles, axis=0).T
            part = jnp.zeros((8, 128), F32)
            for q in range(16):
                zz, yy, cc = q // 8, (q // 2) % 4, q % 2
                piece = block[q * 8 : (q + 1) * 8, :]
                nt[t, cc, yy, zz, :, h * 128 : (h + 1) * 128] = piece
                part = part + piece
            wsum[h] = wsum[h] + part
        if t == 3:
            for h in range(2):
                tot[4 + h : 5 + h, :] = jnp.sum(wsum[h], axis=0, keepdims=True)
            me = y * NC + c
            smy[me] = tot[...]
            for k in (4, 5, 3, 2, 7, 6, 1):
                cp = pltpu.make_async_remote_copy(
                    src_ref=smy.at[me], dst_ref=smy.at[me], send_sem=sent, recv_sem=small_y_in,
                    device_id=at(z, (y + k // 2) % NY, (c + k) % 2), device_id_type=MESH,
                )
                cp.start()
        core_copy(t).start()
        if t == 1:
            pl.semaphore_wait(know.at[3], 1)
            pl.semaphore_wait(know.at[4], 1)
            tell(know.at[5], z_last)

    for t in range(3):
        after_core(t)
    after_core(3)

    def z_copy(t, peer, zz):
        return pltpu.make_async_remote_copy(
            src_ref=nt.at[t, c, y, zz], dst_ref=rz.at[z], send_sem=sent, recv_sem=z_in,
            device_id=at(peer, y, c), device_id_type=MESH,
        )

    def after_y(t):
        arrived(ry.at[t], y_in.at[t])
        nt[t, c, y] = nt[t, c, y] + (ry[t, 0] + ry[t, 1])
        to_each(t, z_copy)

    arrived(smy.at[pl.ds(0, NY * NC - 1)], small_y_in)
    smz[z] = ((smy[0] + smy[1]) + (smy[2] + smy[3])) + ((smy[4] + smy[5]) + (smy[6] + smy[7]))
    for k in (4, 3, 5, 2, 6, 1, 7):
        cp = pltpu.make_async_remote_copy(
            src_ref=smz.at[z], dst_ref=smz.at[z], send_sem=sent, recv_sem=small_z_in,
            device_id=at((z + k) % NZ, y, c), device_id_type=MESH,
        )
        cp.start()
    after_y(0)
    after_y(1)
    after_y(2)
    after_y(3)
    others = pl.ds(0, NZ - 1)
    arrived(rf.at[others], far_z_in)
    total = nt[3, c, y_far, odd]
    for k in range(1, NZ):
        src = (z + k) % NZ
        total = total + rf[src]
    far_sum[0] = total
    far_sent = pltpu.make_async_remote_copy(
        src_ref=far_sum.at[0], dst_ref=far_sum.at[1], send_sem=sent, recv_sem=far_y_in,
        device_id=at(z, y_far, c), device_id_type=MESH,
    )
    far_sent.start()

    arrived(smz.at[others], small_z_in)
    whole = ((smz[0] + smz[1]) + (smz[2] + smz[3])) + ((smz[4] + smz[5]) + (smz[6] + smz[7]))
    inner = K * NZ * NY * NC
    tot[...] = whole
    totals = jnp.concatenate([whole[k : k + 1, :] for k in range(4)], axis=1)
    driver = driver_of(totals * (1.0 / inner))
    rv_ref[...] = jnp.zeros((1, 128), F32) + (
        jnp.sum(totals, axis=1, keepdims=True) * (1.0 / (M * inner))
        + jnp.sum(driver, axis=1, keepdims=True) * (1.0 / M)
    )
    weight = root_t * totals * (1.0 / (M * inner)) + driver / (root_t * M)
    w_hi = weight.astype(BF16).astype(F32)
    w_mid = (weight - w_hi).astype(BF16).astype(F32)
    w_lo = weight - w_hi - w_mid
    rows = lax.broadcasted_iota(jnp.int32, (8, M), 0)
    lhs = jnp.where(rows == 0, w_hi, jnp.where(rows == 1, w_mid, jnp.where(rows == 2, w_lo, 0.0)))
    prod = lax.dot_general(
        lhs.astype(BF16), outer[...], (((1,), (1,)), ((), ())), preferred_element_type=F32
    )
    noise_sum = jnp.sum(prod, axis=0, keepdims=True)
    moment_sum = jnp.concatenate([whole[4:5, :], whole[5:6, :]], axis=1)[:, 0:D]
    rg_ref[...] = (noise_sum + moment_sum * (1.0 / (M * inner))) / (vol_v[...] * start_v[...])
    own_row = tot[pl.ds(path // 16, 1), :] * (1.0 / inner)
    own_row = pltpu.roll(jnp.broadcast_to(own_row, (8, 128)), (128 - (path % 16) * 8) % 128, axis=1)
    pv_ref[...] = own_row[0:1, 0:8]

    arrived(rz.at[others], z_in)
    own = nt[3, c, y, odd]
    for k in range(1, NZ):
        src = (z + k) % NZ
        own = own + rz[src]
    far_sent.wait_recv()
    own = own + far_sum[1]
    pg_ref[...] = own[:, 0:D] * dinv[...]

    rows_sent = 4 * 3 * 8 + 4 * 128 + 4 * 2 * 32 + 2 * 7 * 16 + 2 * 7 * 8 + 16
    arrived(bytes_of.at[pl.ds(0, rows_sent)], sent)


def hand_out(a, b, c, d, a_out, b_out, c_out, d_out, one, sem):
    one[...] = a[0:1, 0:1]
    pairs = ((d, d_out), (b, b_out), (c, c_out), (one, a_out))
    copies = [pltpu.make_async_copy(src, dst, sem.at[k]) for k, (src, dst) in enumerate(pairs)]
    for cp in copies:
        cp.start()
    for cp in copies:
        cp.wait()


def per_device(inner_noise, outer_noise, start, vol, times):
    K, D, M = inner_noise.shape
    hbm = pl.BlockSpec(memory_space=pltpu.HBM)
    vmem = pl.BlockSpec(memory_space=pltpu.VMEM)
    dma = pltpu.SemaphoreType.DMA
    V = pltpu.VMEM
    results = pl.pallas_call(
        kernel,
        out_shape=(V((1, 128), F32), V((1, D), F32), V((1, 8), F32), V((8, D), F32)),
        in_specs=[hbm] * 5,
        out_specs=(vmem,) * 4,
        scratch_shapes=[
            V((4, 256, K, 128), BF16), V((4, K, 256, 128), F32), V((D, M), BF16), V((1, D), F32), V((1, D), F32), V((1, M), F32),
            V((1, 256), F32), V((1, 256), F32), V((264, 128), F32), V((4, 264, 128), F32),
            V((4, K, 128), F32), V((4, 3, K, 128), F32), V((8, M), F32), V((256, 128), F32),
            V((4, NC, NY, 2, 8, 256), F32), V((4, NY, 2, 8, 256), F32),
            V((4, 2, 2, 8, 256), F32), V((NZ, 8, 256), F32), V((NZ, 8, 256), F32), V((2, 8, 256), F32), V((1216, 128), F32),
            V((NY * NC, 8, 128), F32), V((NZ, 8, 128), F32), V((8, 128), F32),
            V((8, D), F32),
            dma((8,)), dma, dma((4,)), dma((4,)), dma((4,)), dma, dma, dma, dma, dma,
            pltpu.SemaphoreType.REGULAR((6,)),
        ],
        compiler_params=pltpu.CompilerParams(
            collective_id=0, has_side_effects=True
        ),
    )(
        jnp.transpose(inner_noise, (1, 0, 2)), outer_noise, start[None], vol[None], times[None]
    )
    root_value, root_grad, point_value, point_grad = pl.pallas_call(
        hand_out,
        out_shape=tuple(jax.ShapeDtypeStruct(s, F32) for s in ((1, 1), (1, D), (1, 8), (8, D))),
        in_specs=[vmem] * 4,
        out_specs=(hbm,) * 4,
        scratch_shapes=[V((1, 1), F32), dma((4,))],
        compiler_params=pltpu.CompilerParams(vmem_limit_bytes=1024 * 1024),
    )(*results)
    return root_value[0], root_grad[0], point_value[0], point_grad.T


def solution(mesh):
    in_specs = (P("path", "dim", None), P("dim", None), P("dim"), P("dim"), P())
    out_specs = (P(), P("dim"), P("path"), P("dim", "path"))
    return jax.shard_map(
        per_device, mesh=mesh, in_specs=in_specs, out_specs=out_specs, check_vma=False
    )
```

```python
import functools

import jax
import jax.numpy as jnp
from jax import lax
from jax.experimental import pallas as pl
from jax.experimental.pallas import tpu as pltpu
from jax.sharding import PartitionSpec as P

drift = 0.02
delta = 2.0 / 3.0
rate_free = 0.02
gamma_high = 0.2
gamma_low = 0.02
value_high = 0.4
value_low = 0.7

NX, NY, NZ, NC = 4, 4, 8, 2
MESH = pl.DeviceIdType.MESH
F32 = jnp.float32
BF16 = jnp.bfloat16
CHUNKS = 5


def driver_of(value):
    slope = jnp.clip((value - value_high) / (value_low - value_high), 0.0, 1.0)
    quota = gamma_high + (gamma_low - gamma_high) * slope
    return -(1.0 - delta) * quota * value - rate_free * value


def smallest(terms):
    while len(terms) > 1:
        pairs = [jnp.minimum(a, b) for a, b in zip(terms[::2], terms[1::2])]
        terms = pairs + terms[len(pairs) * 2 :]
    return terms[0]


def kernel(
    noise_hbm, outer_hbm, start_hbm, vol_hbm, times_hbm,
    rv_ref, rg_ref, pv_ref, pg_ref,
    noise, turned, outer, start_v, vol_v, times_v,
    startp, volp, volb, abase, lmin, rx, rows_t, stage, nt, rc, ry, rz, rf, far_sum, bytes_of, smy, smz, tot, dinv,
    in_sem, sent, x_in, core_in, y_in, z_in, far_z_in, far_y_in, small_y_in, small_z_in, know,
):
    D, K, M = noise_hbm.shape
    path = lax.axis_index("path")
    x = lax.axis_index("dim")
    z = path // (NY * NC)
    y = (path // NC) % NY
    c = path % NC
    jz = z // 2

    def at_x(k):
        return (path, (x + k) % NX)

    def at(zz, yy, cc):
        return ((zz * NY + yy) * NC + cc, x)

    small_in = [
        pltpu.make_async_copy(vol_hbm, vol_v, in_sem.at[0]),
        pltpu.make_async_copy(start_hbm, start_v, in_sem.at[1]),
        pltpu.make_async_copy(times_hbm, times_v, in_sem.at[2]),
    ]
    for cp in small_in:
        cp.start()
    odd = z % 2
    blocks = [(jz + off) % 4 for off in (2, 1 + 2 * odd, 3 - 2 * odd, 0)]

    def lanes_of(t):
        return pl.ds(pl.multiple_of(blocks[t] * 128, 128), 128)

    per = D // CHUNKS
    noise_in = [
        [
            pltpu.make_async_copy(
                noise_hbm.at[pl.ds(q * per, per), :, lanes_of(t)],
                noise.at[t, pl.ds(q * per, per)],
                in_sem.at[4 + min(t, 2)],
            )
            for q in range(CHUNKS)
        ]
        for t in range(4)
    ]
    outer_in = pltpu.make_async_copy(outer_hbm, outer, in_sem.at[3])
    outer_in.start()
    for cp in noise_in[0]:
        cp.start()

    barrier = pltpu.get_barrier_semaphore()
    near = [at((z + k) % NZ, y, c) for k in (1, NZ - 1)]
    near += [at(z, (y + k) % NY, cc) for k in (1, NY - 1) for cc in (c, 1 - c)]
    near += [at_x(k) for k in (1, 2, 3)] + [at(z, y, 1 - c)]
    for peer in near:
        pl.semaphore_signal(barrier, inc=1, device_id=peer, device_id_type=MESH)

    def tell(sem, peer):
        pl.semaphore_signal(sem, inc=1, device_id=peer, device_id_type=MESH)

    z_next, z_last = at((z + 1) % NZ, y, c), at((z + NZ - 1) % NZ, y, c)

    for t in range(1, 4):
        for cp in noise_in[t]:
            cp.start()
    for t in range(4):
        noise[t, D:] = jnp.zeros((256 - D, K, 128), BF16)
    for cp in small_in:
        cp.wait()

    startp[...] = jnp.ones_like(startp)
    volp[...] = jnp.ones_like(volp)
    startp[:, 0:D] = start_v[...]
    volp[:, 0:D] = vol_v[...]
    vol = volp[...]
    begin = startp[...]
    times = times_v[...]
    tau = 1.0 - times
    root_t = jnp.sqrt(times)
    root_tau = jnp.sqrt(tau)
    inv_root_tau = 1.0 / root_tau
    offset = jnp.log(begin) + (drift - 0.5 * vol * vol)
    for h in range(2):
        volb[h * 128 : (h + 1) * 128, :] = jnp.broadcast_to(
            vol[:, h * 128 : (h + 1) * 128], (128, 128)
        ).T
        stage[h * 128 : (h + 1) * 128, :] = jnp.broadcast_to(
            offset[:, h * 128 : (h + 1) * 128], (128, 128)
        ).T
    rows_t[0:1, :] = root_t
    rows_t[1:2, :] = root_tau
    rows_t[2:3, :] = inv_root_tau

    def coefficients(t):
        scale = rows_t[0:1, lanes_of(t)]
        inv = rows_t[2:3, lanes_of(t)]
        for lo in range(0, D, 16):
            hi = min(lo + 16, D)
            o = outer[lo:hi, lanes_of(t)].astype(F32)
            abase[t, lo:hi, :] = (stage[lo:hi, :] + volb[lo:hi, :] * (scale * o)) * inv

    def arrived(ref, sem):
        pltpu.make_async_copy(ref, ref, sem).wait()

    def x_copy(t, k):
        return pltpu.make_async_remote_copy(
            src_ref=lmin.at[t], dst_ref=rx.at[t, k - 1], send_sem=sent, recv_sem=x_in.at[min(t, 2)],
            device_id=at_x(k), device_id_type=MESH,
        )

    def minimum_of(ts):
        here = noise.at[pl.ds(ts[0], len(ts)), pl.ds(0, D)]
        pltpu.make_async_copy(here, here, in_sem.at[4 + ts[0]]).wait()
        acc = [jnp.full((K, 128), 3.0e38, F32) for _ in ts]
        for q in range(CHUNKS):
            terms = [[] for _ in ts]
            for d in range(q * per, (q + 1) * per):
                v = volb[pl.ds(d, K, stride=0), :]
                for row, t in zip(terms, ts):
                    row.append(noise[t, d].astype(F32) * v + abase[t, pl.ds(d, K, stride=0), :])
            acc = [jnp.minimum(a, smallest(r)) for a, r in zip(acc, terms)]
        for t, a in zip(ts, acc):
            lmin[t] = a

    outer_in.wait()
    for t in range(4):
        coefficients(t)
    for ts in ((0,), (1,), (2, 3)):
        minimum_of(ts)
        if ts[0] == 0:
            pl.semaphore_wait(barrier, len(near))
            tell(know.at[0], at(z, (y + NY - 1) % NY, c))
            tell(know.at[1], z_last)
            tell(know.at[2], z_next)
        for t in ts:
            for k in (2, 1, 3):
                x_copy(t, k).start()

    lane = lax.broadcasted_iota(jnp.int32, (K, M), 1)
    row = lax.broadcasted_iota(jnp.int32, (K, M), 0)
    pick = lane == path * K + row
    own_t = jnp.sum(jnp.where(pick, times, 0.0), axis=1, keepdims=True)
    own_outer = lax.dot_general(
        jnp.where(pick, 1.0, 0.0).astype(BF16), outer[...], (((1,), (1,)), ((), ())),
        preferred_element_type=F32,
    )
    vol_d = vol_v[...]
    own_state = start_v[...] * jnp.exp(
        (drift - 0.5 * vol_d * vol_d) * own_t + vol_d * jnp.sqrt(own_t) * own_outer
    )
    dinv[...] = 1.0 / ((K * NZ * NY * NC) * vol_d * own_state * (1.0 - own_t))

    pl.semaphore_wait(know.at[0], 1)
    pl.semaphore_wait(know.at[1], 1)
    pl.semaphore_wait(know.at[2], 1)
    tell(know.at[3], z_last)
    tell(know.at[4], z_next)

    sub = lax.broadcasted_iota(jnp.int32, (8, 128), 0)

    def swapped(tiles, step):
        low = (sub & step) == 0
        out = list(tiles)
        for a in range(8):
            if a & step == 0:
                lo, hi = tiles[a], tiles[a + step]
                out[a] = jnp.where(low, lo, pltpu.roll(hi, step, axis=0))
                out[a + step] = jnp.where(low, pltpu.roll(lo, 8 - step, axis=0), hi)
        return out

    for t in range(4):

        def turn(r, _, t=t):
            for u in range(4):
                g = r * 4 + u
                tiles = [noise[t, g * 8 + s].astype(F32) for s in range(8)]
                for step in (4, 2, 1):
                    tiles = swapped(tiles, step)
                for k in range(8):
                    turned[t, k, pl.ds(pl.multiple_of(g * 8, 8), 8), :] = tiles[k]
            return 0

        lax.fori_loop(0, 8, turn, 0)

    def core_copy(t):
        return pltpu.make_async_remote_copy(
            src_ref=nt.at[t, 1 - c], dst_ref=rc.at[t], send_sem=sent, recv_sem=core_in.at[t],
            device_id=at(z, y, 1 - c), device_id_type=MESH,
        )

    side = {1: 0, 3: 1}
    y_far = (y + 2) % NY

    def y_copy(t, k):
        peer = (y + k) % NY
        return pltpu.make_async_remote_copy(
            src_ref=nt.at[t, c, peer], dst_ref=ry.at[t, side[k]],
            send_sem=sent, recv_sem=y_in.at[t],
            device_id=at(z, peer, c), device_id_type=MESH,
        )

    def far_copy(t, peer, zz):
        return pltpu.make_async_remote_copy(
            src_ref=nt.at[t, c, y_far, zz], dst_ref=rf.at[z], send_sem=sent, recv_sem=far_z_in,
            device_id=at(peer, y, c), device_id_type=MESH,
        )

    def to_each(t, copy):
        if t == 3:
            copy(t, 2 * blocks[t] + 1 - odd, 1 - odd).start()
        else:
            for zz in range(2):
                copy(t, 2 * blocks[t] + zz, zz).start()

    def after_core(t):
        arrived(rc.at[t], core_in.at[t])
        nt[t, c] = nt[t, c] + rc[t]
        if t == 0:
            pl.semaphore_wait(know.at[5], 1)
        to_each(t, far_copy)
        for k in (1, 3):
            y_copy(t, k).start()

    wsum = [jnp.zeros((8, 128), F32)] * 2
    tot[...] = jnp.zeros_like(tot)
    for t, j in enumerate(blocks):
        if t < 2:
            arrived(rx.at[t], x_in.at[t])
        elif t == 2:
            arrived(rx.at[pl.ds(2, 2)], x_in.at[2])
        least = jnp.minimum(
            jnp.minimum(lmin[t], rx[t, 0]), jnp.minimum(rx[t, 1], rx[t, 2])
        )
        scale = rows_t[1:2, lanes_of(t)]
        payoff = jnp.exp(scale * least)
        p = payoff * scale
        tot[pl.ds(j, 1), :] = jnp.sum(payoff, axis=0, keepdims=True)
        rows = [jnp.broadcast_to(p[k : k + 1, :], (8, 128)) for k in range(K)]
        for h in range(2):
            tiles = []
            for g in range(16):
                first = h * 128 + g * 8
                terms = [turned[t, k, first : first + 8, :] * rows[k] for k in range(K)]
                while len(terms) > 1:
                    terms = [a + b for a, b in zip(terms[::2], terms[1::2])]
                tiles.append(terms[0])
            block = jnp.concatenate(tiles, axis=0).T
            part = jnp.zeros((8, 128), F32)
            for q in range(16):
                zz, yy, cc = q // 8, (q // 2) % 4, q % 2
                piece = block[q * 8 : (q + 1) * 8, :]
                nt[t, cc, yy, zz, :, h * 128 : (h + 1) * 128] = piece
                part = part + piece
            wsum[h] = wsum[h] + part
        if t == 3:
            for h in range(2):
                tot[4 + h : 5 + h, :] = jnp.sum(wsum[h], axis=0, keepdims=True)
            me = y * NC + c
            smy[me] = tot[...]
            for k in (4, 5, 3, 2, 7, 6, 1):
                cp = pltpu.make_async_remote_copy(
                    src_ref=smy.at[me], dst_ref=smy.at[me], send_sem=sent, recv_sem=small_y_in,
                    device_id=at(z, (y + k // 2) % NY, (c + k) % 2), device_id_type=MESH,
                )
                cp.start()
        core_copy(t).start()
        if t == 1:
            pl.semaphore_wait(know.at[3], 1)
            pl.semaphore_wait(know.at[4], 1)
            tell(know.at[5], z_last)

    for t in range(3):
        after_core(t)
    after_core(3)

    def z_copy(t, peer, zz):
        return pltpu.make_async_remote_copy(
            src_ref=nt.at[t, c, y, zz], dst_ref=rz.at[z], send_sem=sent, recv_sem=z_in,
            device_id=at(peer, y, c), device_id_type=MESH,
        )

    def after_y(t):
        arrived(ry.at[t], y_in.at[t])
        nt[t, c, y] = nt[t, c, y] + (ry[t, 0] + ry[t, 1])
        to_each(t, z_copy)

    arrived(smy.at[pl.ds(0, NY * NC - 1)], small_y_in)
    smz[z] = ((smy[0] + smy[1]) + (smy[2] + smy[3])) + ((smy[4] + smy[5]) + (smy[6] + smy[7]))
    for k in (4, 3, 5, 2, 6, 1, 7):
        cp = pltpu.make_async_remote_copy(
            src_ref=smz.at[z], dst_ref=smz.at[z], send_sem=sent, recv_sem=small_z_in,
            device_id=at((z + k) % NZ, y, c), device_id_type=MESH,
        )
        cp.start()
    after_y(0)
    after_y(1)
    after_y(2)
    after_y(3)
    others = pl.ds(0, NZ - 1)
    arrived(rf.at[others], far_z_in)
    total = nt[3, c, y_far, odd]
    for k in range(1, NZ):
        src = (z + k) % NZ
        total = total + rf[src]
    far_sum[0] = total
    far_sent = pltpu.make_async_remote_copy(
        src_ref=far_sum.at[0], dst_ref=far_sum.at[1], send_sem=sent, recv_sem=far_y_in,
        device_id=at(z, y_far, c), device_id_type=MESH,
    )
    far_sent.start()

    arrived(smz.at[others], small_z_in)
    whole = ((smz[0] + smz[1]) + (smz[2] + smz[3])) + ((smz[4] + smz[5]) + (smz[6] + smz[7]))
    inner = K * NZ * NY * NC
    tot[...] = whole
    totals = jnp.concatenate([whole[k : k + 1, :] for k in range(4)], axis=1)
    driver = driver_of(totals * (1.0 / inner))
    rv_ref[...] = jnp.zeros((1, 128), F32) + (
        jnp.sum(totals, axis=1, keepdims=True) * (1.0 / (M * inner))
        + jnp.sum(driver, axis=1, keepdims=True) * (1.0 / M)
    )
    weight = root_t * totals * (1.0 / (M * inner)) + driver / (root_t * M)
    w_hi = weight.astype(BF16).astype(F32)
    w_mid = (weight - w_hi).astype(BF16).astype(F32)
    w_lo = weight - w_hi - w_mid
    rows = lax.broadcasted_iota(jnp.int32, (8, M), 0)
    lhs = jnp.where(rows == 0, w_hi, jnp.where(rows == 1, w_mid, jnp.where(rows == 2, w_lo, 0.0)))
    prod = lax.dot_general(
        lhs.astype(BF16), outer[...], (((1,), (1,)), ((), ())), preferred_element_type=F32
    )
    noise_sum = jnp.sum(prod, axis=0, keepdims=True)
    moment_sum = jnp.concatenate([whole[4:5, :], whole[5:6, :]], axis=1)[:, 0:D]
    rg_ref[...] = (noise_sum + moment_sum * (1.0 / (M * inner))) / (vol_v[...] * start_v[...])
    own_row = tot[pl.ds(path // 16, 1), :] * (1.0 / inner)
    own_row = pltpu.roll(jnp.broadcast_to(own_row, (8, 128)), (128 - (path % 16) * 8) % 128, axis=1)
    pv_ref[...] = own_row[0:1, 0:8]

    arrived(rz.at[others], z_in)
    own = nt[3, c, y, odd]
    for k in range(1, NZ):
        src = (z + k) % NZ
        own = own + rz[src]
    far_sent.wait_recv()
    own = own + far_sum[1]
    pg_ref[...] = own[:, 0:D] * dinv[...]

    rows_sent = 4 * 3 * 8 + 4 * 128 + 4 * 2 * 32 + 2 * 7 * 16 + 2 * 7 * 8 + 16
    arrived(bytes_of.at[pl.ds(0, rows_sent)], sent)


def hand_out(a, b, c, d, a_out, b_out, c_out, d_out, one, sem):
    one[...] = a[0:1, 0:1]
    pairs = ((d, d_out), (b, b_out), (c, c_out), (one, a_out))
    copies = [pltpu.make_async_copy(src, dst, sem.at[k]) for k, (src, dst) in enumerate(pairs)]
    for cp in copies:
        cp.start()
    for cp in copies:
        cp.wait()


def per_device(inner_noise, outer_noise, start, vol, times):
    K, D, M = inner_noise.shape
    hbm = pl.BlockSpec(memory_space=pltpu.HBM)
    vmem = pl.BlockSpec(memory_space=pltpu.VMEM)
    dma = pltpu.SemaphoreType.DMA
    V = pltpu.VMEM
    results = pl.pallas_call(
        kernel,
        out_shape=(V((1, 128), F32), V((1, D), F32), V((1, 8), F32), V((8, D), F32)),
        in_specs=[hbm] * 5,
        out_specs=(vmem,) * 4,
        scratch_shapes=[
            V((4, 256, K, 128), BF16), V((4, K, 256, 128), F32), V((D, M), BF16), V((1, D), F32), V((1, D), F32), V((1, M), F32),
            V((1, 256), F32), V((1, 256), F32), V((256, 128), F32), V((4, 256, 128), F32),
            V((4, K, 128), F32), V((4, 3, K, 128), F32), V((8, M), F32), V((256, 128), F32),
            V((4, NC, NY, 2, 8, 256), F32), V((4, NY, 2, 8, 256), F32),
            V((4, 2, 2, 8, 256), F32), V((NZ, 8, 256), F32), V((NZ, 8, 256), F32), V((2, 8, 256), F32), V((1216, 128), F32),
            V((NY * NC, 8, 128), F32), V((NZ, 8, 128), F32), V((8, 128), F32),
            V((8, D), F32),
            dma((7,)), dma, dma((3,)), dma((4,)), dma((4,)), dma, dma, dma, dma, dma,
            pltpu.SemaphoreType.REGULAR((6,)),
        ],
        compiler_params=pltpu.CompilerParams(
            collective_id=0, has_side_effects=True
        ),
    )(
        jnp.transpose(inner_noise, (1, 0, 2)), outer_noise, start[None], vol[None], times[None]
    )
    root_value, root_grad, point_value, point_grad = pl.pallas_call(
        hand_out,
        out_shape=tuple(jax.ShapeDtypeStruct(s, F32) for s in ((1, 1), (1, D), (1, 8), (8, D))),
        in_specs=[vmem] * 4,
        out_specs=(hbm,) * 4,
        scratch_shapes=[V((1, 1), F32), dma((4,))],
        compiler_params=pltpu.CompilerParams(vmem_limit_bytes=1024 * 1024),
    )(*results)
    return root_value[0], root_grad[0], point_value[0], point_grad.T


def solution(mesh):
    in_specs = (P("path", "dim", None), P("dim", None), P("dim"), P("dim"), P())
    out_specs = (P(), P("dim"), P("path"), P("dim", "path"))
    return jax.shard_map(
        per_device, mesh=mesh, in_specs=in_specs, out_specs=out_specs, check_vma=False
    )
```
